256 devices in a mesh: rows: 8 (over y, core), cols: 16 (over z_hi, x), hub: 2 (over z_lo).
Axes of the slice: x: 4, y: 4, z: 8 (z_hi: 4, z_lo: 2; z = z_hi * 2 + z_lo), core: 2. Of those that a mesh axis runs over, the one named last changes fastest.
Arguments:
- light_bits: int32 [384, 12288], P('rows', 'cols'), may hold values from -2147483648 to 2147483647, as said below
- hub_bits: int32 [8, 12288], P('hub', 'cols'), may hold values from -2147483648 to 2147483647, as said below
- hub_ids: int32 [256], replicated, may hold values from 0 to 12287, as said below
Outputs:
- clustering: float32 [12288], P(('rows', 'cols'))
The draws below stay inside these ranges and needn't reach their ends.
Inputs may be any that keep to these rules, and one draw needn't show every extreme that they name: Every word holds 32 bits; the matrix of light_bits is symmetric with a zero diagonal. `hub_bits`: every word holds 32 bits. `hub_ids`: 256 distinct vertex numbers.
All inputs are finite; a program needn't handle non-finite values.
Results may differ from the reference program's by a relative error of at most 0.0003.
Values sent between devices are 32-bit elements; how exact they have to be, the bound alone decides.
No kernel may reach another device: no remote copies, remote signals or barrier semaphores. Data moves between devices by JAX's collectives and lax.ppermute only.
A program may use at most 128 MiB of HBM per device.

```python
import jax
import jax.numpy as jnp
from jax import lax

VERTICES = 12288
HUBS = 256


def vertex_weights(key):
    vertex_rank = jax.random.permutation(jax.random.fold_in(key, 7), VERTICES).astype(jnp.int32)
    weight = 4 + 128 // (1 + vertex_rank // 32)
    return (vertex_rank, weight)


def pack_bits(linked):
    powers = jnp.left_shift(jnp.int32(1), jnp.arange(32, dtype=jnp.int32))
    grouped = linked.astype(jnp.int32).reshape(linked.shape[0] // 32, 32, linked.shape[1])
    return jnp.sum(grouped * powers[None, :, None], axis=1).astype(jnp.int32)


def draw_light_bits(key, part):
    vertex_rank, weight = vertex_weights(key)
    samples = jax.random.randint(jax.random.fold_in(key, 11), (VERTICES, VERTICES), 0, 8192, dtype=jnp.int32)
    linked = samples < weight[:, None] * weight[None, :]
    vertex_ids = jnp.arange(VERTICES, dtype=jnp.int32)
    one_side = jnp.logical_and(linked, vertex_ids[None, :] > vertex_ids[:, None])
    symmetric = jnp.logical_or(one_side, one_side.T)
    return pack_bits(symmetric)


def draw_hub_bits(key, part):
    vertex_rank, weight = vertex_weights(key)
    samples = jax.random.randint(jax.random.fold_in(key, 13), (HUBS, VERTICES), 0, 1024, dtype=jnp.int32)
    linked = samples < 48 + weight[None, :]
    return pack_bits(linked)


def draw_hub_ids(key, part):
    vertex_rank, weight = vertex_weights(key)
    by_rank = jnp.argsort(vertex_rank)
    return by_rank[:HUBS].astype(jnp.int32)


def setup_inputs(seed: int = 0) -> dict:
    streams_of = jax.random.split(jax.random.key(seed), 4)
    return {
        "light_bits": draw_light_bits(jax.random.fold_in(streams_of[3], 71), 0),
        "hub_bits": draw_hub_bits(jax.random.fold_in(streams_of[3], 71), 0),
        "hub_ids": draw_hub_ids(jax.random.fold_in(streams_of[3], 71), 0),
    }


def unpack(packed):
    shifts = jnp.arange(32, dtype=jnp.int32)
    bit_grid = jnp.bitwise_and(jnp.right_shift(packed[:, None, :], shifts[None, :, None]), 1)
    return bit_grid.reshape(packed.shape[0] * 32, packed.shape[1]).astype(jnp.float32)


def reference(light_bits, hub_bits, hub_ids):
    total = light_bits.shape[1]
    vertex_ids = jnp.arange(total, dtype=jnp.int32)
    is_hub = jnp.any(vertex_ids[:, None] == hub_ids[None, :], axis=1)
    light = jnp.where(is_hub, 0.0, 1.0).astype(jnp.float32)
    adjacency = unpack(light_bits) * light[:, None] * light[None, :]
    two_paths = jnp.dot(adjacency, adjacency, precision=lax.Precision.HIGHEST, preferred_element_type=jnp.float32)
    light_tri = 0.5 * jnp.sum(adjacency * two_paths, axis=1)
    hub_rows = unpack(hub_bits) * light[None, :]
    reach_hub = jnp.dot(hub_rows, adjacency, precision=lax.Precision.HIGHEST, preferred_element_type=jnp.float32)
    intersect = hub_rows * reach_hub
    hub_tri = 0.5 * jnp.sum(intersect, axis=1)
    hub_deg = jnp.sum(hub_rows, axis=1)
    owners = (vertex_ids[:, None] == hub_ids[None, :]).astype(jnp.float32)
    triangles = light_tri + jnp.sum(intersect, axis=0) + jnp.sum(owners * hub_tri[None, :], axis=1)
    degrees = jnp.sum(adjacency, axis=1) + jnp.sum(hub_rows, axis=0) + jnp.sum(owners * hub_deg[None, :], axis=1)
    return triangles / (1.0 + degrees)
```

```python
import functools

import jax
import jax.numpy as jnp
from jax import lax
from jax.experimental import pallas as pl
from jax.experimental.pallas import tpu as pltpu
from jax.sharding import Mesh
from jax.sharding import PartitionSpec as P

AXES = ("y", "core", "zh", "x", "zl")
ROWS = ("y", "core")
COLS = ("zh", "x")
SIZES = (4, 2, 4, 4, 2)
F8 = jnp.float8_e4m3fn
F32 = jnp.float32
I32 = jnp.int32
BITS = 8
OUT = 96


def flat(y, core, zh, x, zl):
    return (((y * 2 + core) * 4 + zh) * 4 + x) * 2 + zl


def permutation(source_of):
    pairs = []
    for y in range(4):
        for core in range(2):
            for zh in range(4):
                for x in range(4):
                    for zl in range(2):
                        s = source_of(y, core, zh, x, zl)
                        if s is not None:
                            pairs.append((flat(*s), flat(y, core, zh, x, zl)))
    return pairs


def slots(zh, zl):
    return ((zh + zl) % 4, (zh + 3 + 3 * zl) % 4)


def z_near(y, core, zh, x, zl):
    return (y, core, (zh + 3) % 4, x, 1) if zl == 0 else (y, core, (zh + 1) % 4, x, 0)


def z_far(y, core, zh, x, zl):
    return None if zl == 0 else (y, core, (zh + 2) % 4, x, 0)


def y_out(y, core, zh, x, zl):
    a, b = slots(zh, zl)
    away = 1 if zl == 0 else 3
    if y == (a + away) % 4:
        return (a, core, zh, x, zl)
    if y == (b - away) % 4:
        return (b, core, zh, x, zl)
    return None


def y_swap(y, core, zh, x, zl):
    a, b = slots(zh, zl)
    away = 1 if zl == 0 else 3
    oa, ob = (a + away) % 4, (b - away) % 4
    return ({a: b, b: a, oa: ob, ob: oa}[y], core, zh, x, zl)


def hub_source(second):
    def source(y, core, zh, x, zl):
        row, col = 2 * y + core, 4 * zh + x
        side = (col // 8) ^ second
        c = 2 * row + side
        r = col % 8
        return (r // 2, r % 2, c // 4, c % 4, zl)

    return source


def unpack(words, dtype):
    n = words.shape[1]
    shifts = lax.broadcasted_iota(I32, (32, n), 0)
    rows = [
        jnp.right_shift(jnp.broadcast_to(words[i : i + 1, :], (32, n)), shifts) & 1
        for i in range(words.shape[0])
    ]
    return jnp.concatenate(rows, 0).astype(F32).astype(dtype)


def find_keep(idc, idr, keep):
    q = (lax.broadcasted_iota(I32, (16, 256), 0) == idr[...] // 768).astype(jnp.bfloat16)
    r = (lax.broadcasted_iota(I32, (256, 768), 1) == idc[...] % 768).astype(jnp.bfloat16)
    count = jnp.dot(q, r, preferred_element_type=F32)
    keep[...] = jnp.where(count > 0.5, 0, -1)


def place():
    y, core = lax.axis_index("y"), lax.axis_index("core")
    zh, x, zl = lax.axis_index("zh"), lax.axis_index("x"), lax.axis_index("zl")
    return y, core, zh, x, zl


def light_kernel(idc, idr, own, r0, rp, rm, r2, yy, yc, tri, deg, keep, lhs, rhs):
    y, core, zh, x, zl = place()
    row, col = 2 * y + core, 4 * zh + x
    groups = (lax.rem(zh + zl, 4), lax.rem(zh + 3 + 3 * zl, 4))
    find_keep(idc, idr, keep)
    w = (lax.broadcasted_iota(I32, (48, 256), 0) + 48 * row == idr[...] // 32).astype(jnp.bfloat16)
    b = (lax.broadcasted_iota(I32, (256, 32), 1) == idc[...] % 32).astype(jnp.bfloat16)
    light = 1.0 - jnp.dot(w, b, preferred_element_type=F32)
    sources = ((r0, 0), (rp, 1), (rm, 3), (r2, 2))
    for n, (ref, rel) in enumerate(sources):
        xs = lax.rem(x + rel, 4)
        other = (xs // 2) != core
        for s in range(2):
            at = pl.multiple_of(48 * s + 24 * lax.rem(xs, 2), 8)
            words = jnp.where(other, yc[pl.ds(at, 24), :], yy[pl.ds(at, 24), :])
            base = (2 * n + s) * 768
            for part in range(3):
                rhs[base + 256 * part : base + 256 * part + 256, :] = unpack(
                    words[8 * part : 8 * part + 8, :], F8
                )
    mine = own[...] & keep[pl.ds(col, 1), :]
    for t in range(32 // BITS):
        for n, (ref, rel) in enumerate(sources):
            xs = lax.rem(x + rel, 4)
            for s in range(2):
                words = ref[48 * s : 48 * s + 48, :] & keep[pl.ds(4 * groups[s] + xs, 1), :]
                bits = jnp.concatenate(
                    [jnp.right_shift(words, t * BITS + b) & 1 for b in range(BITS)], 0
                )
                base = (2 * n + s) * 768
                lhs[t % 2, :, base : base + 768] = bits.astype(F32).astype(F8)
        paths = jnp.dot(lhs[t % 2], rhs[...], preferred_element_type=F32)
        for b in range(BITS):
            at = t * BITS + b
            edge = (jnp.right_shift(mine, at) & 1).astype(F32)
            closed = paths[48 * b : 48 * b + 48, :] * edge
            tri[:, at : at + 1] = jnp.sum(closed, axis=1, keepdims=True)
            deg[:, at : at + 1] = jnp.sum(edge, axis=1, keepdims=True)
    first = (zl == 0).astype(F32)
    tri[...] = 0.5 * tri[...] * light
    deg[...] = first * deg[...] * light


def hub_kernel(idc, idr, own, hub, h1, h2, tri, deg, table, keep, near):
    y, core, zh, x, zl = place()
    row, col = 2 * y + core, 4 * zh + x
    find_keep(idc, idr, keep)
    kc = keep[pl.ds(col, 1), :]
    mine = own[...] & kc
    for part in range(6):
        near[256 * part : 256 * part + 256, :] = unpack(mine[8 * part : 8 * part + 8, :], F8)
    swap = col >= 8
    ha = jnp.where(swap, h2[...], h1[...]) & keep[pl.ds(2 * row, 1), :]
    hb = jnp.where(swap, h1[...], h2[...]) & keep[pl.ds(2 * row + 1, 1), :]
    here = unpack(jnp.concatenate([ha, hb], axis=1), F32)
    cols = unpack(hub[...] & kc, F32)
    reach = lax.dot_general(
        cols.astype(F8), near[...], (((1,), (1,)), ((), ())), preferred_element_type=F32
    )
    both = here * reach
    tri[...] = jnp.sum(both, axis=0, keepdims=True)
    deg[...] = (col == 0).astype(F32) * jnp.sum(here, axis=0, keepdims=True)
    hub_tri = 0.5 * jnp.sum(both, axis=1, keepdims=True)
    hub_deg = (row == 0).astype(F32) * jnp.sum(cols, axis=1, keepdims=True)
    at = pl.multiple_of(zl * 128, 128)
    ids = idc[pl.ds(at, 128), :]
    lane = lax.broadcasted_iota(I32, (128, 128), 1)
    inside = lane == ids % OUT
    block = (lax.broadcasted_iota(I32, (128, 128), 1) == ids // OUT).astype(F32)
    for n, value in enumerate((hub_tri, hub_deg)):
        spread = jnp.where(inside, value, 0.0)
        table[:, 128 * n : 128 * n + 128] = lax.dot_general(
            block,
            spread,
            (((0,), (0,)), ((), ())),
            precision=lax.Precision.HIGHEST,
            preferred_element_type=F32,
        )


def call(kernel, outs, scratch, args, flops):
    vmem = pl.BlockSpec(memory_space=pltpu.VMEM)
    return pl.pallas_call(
        kernel,
        out_shape=[jax.ShapeDtypeStruct(s, F32) for s in outs],
        in_specs=[vmem] * len(args),
        out_specs=[vmem] * len(outs),
        scratch_shapes=scratch,
        cost_estimate=pl.CostEstimate(flops=flops, bytes_accessed=1 << 20, transcendentals=0),
        compiler_params=pltpu.CompilerParams(vmem_limit_bytes=56 * 2**20),
    )(*args)


def body(light_bits, hub_bits, hub_ids):
    y, core, zh, x, zl = place()
    row = 2 * y + core
    idc, idr = hub_ids[:, None], hub_ids[None, :]
    send = functools.partial(lax.ppermute, axis_name=AXES)
    near = send(light_bits, perm=permutation(z_near))
    far = send(light_bits, perm=permutation(z_far))
    even = zl == 0
    group = jnp.concatenate([jnp.where(even, light_bits, near), jnp.where(even, near, far)], 0)
    ring = [
        lax.ppermute(group, "x", [((d + r) % 4, d) for d in range(4)]) for r in (1, 3, 2)
    ]
    out = send(light_bits, perm=permutation(y_out))
    ga, gb = (zh + zl) % 4, (zh + 3 + 3 * zl) % 4
    root = (y == ga) | (y == gb)
    have = jnp.where(root, light_bits, out)
    got = send(have, perm=permutation(y_swap))
    first = (y == ga) | (y == (ga + 1 + 2 * zl) % 4)
    yy = jnp.concatenate([jnp.where(first, have, got), jnp.where(first, got, have)], 0)
    yc = lax.ppermute(yy, "core", [(0, 1), (1, 0)])
    h1 = send(hub_bits, perm=permutation(hub_source(0)))
    h2 = send(hub_bits, perm=permutation(hub_source(1)))
    htri, hdeg, table = call(
        hub_kernel,
        [(1, 1536), (1, 1536), (128, 256)],
        [pltpu.VMEM((16, 768), I32), pltpu.VMEM((1536, 768), F8)],
        (idc, idr, light_bits, hub_bits, h1, h2),
        1 << 29,
    )
    tri, deg = call(
        light_kernel,
        [(48, 32), (48, 32)],
        [
            pltpu.VMEM((16, 768), I32),
            pltpu.VMEM((2, 48 * BITS, 6144), F8),
            pltpu.VMEM((6144, 768), F8),
        ],
        (idc, idr, light_bits, group, *ring, yy, yc),
        1 << 33,
    )
    tri = tri.reshape(16, OUT) + htri.reshape(16, OUT)
    deg = deg.reshape(16, OUT) + hdeg.reshape(16, OUT)
    pad = jnp.zeros((16, 128 - OUT), F32)
    mine = jnp.concatenate([tri, pad, deg, pad], 1)
    table = lax.dynamic_update_slice_in_dim(
        table, lax.dynamic_slice_in_dim(table, 16 * row, 16, 0) + mine, 16 * row, 0
    )
    table = jnp.broadcast_to(table[:, None, :], (128, 2, 256)).reshape(256, 256)
    everyone = lax.all_to_all(table, AXES, 0, 0, tiled=True)
    total = jnp.sum(everyone, axis=0)
    return total[:OUT] / (1.0 + total[128 : 128 + OUT])


def solution(mesh):
    finer = Mesh(mesh.devices.reshape(SIZES), AXES)
    placed = (P(ROWS, COLS), P("zl", COLS), P())
    return jax.shard_map(
        body, mesh=finer, in_specs=placed, out_specs=P(ROWS + COLS), check_vma=False
    )
```

```python
import functools

import jax
import jax.numpy as jnp
from jax import lax
from jax.experimental import pallas as pl
from jax.experimental.pallas import tpu as pltpu
from jax.sharding import Mesh
from jax.sharding import PartitionSpec as P

AXES = ("y", "core", "zh", "x", "zl")
ROWS = ("y", "core")
COLS = ("zh", "x")
SIZES = (4, 2, 4, 4, 2)
F8 = jnp.float8_e4m3fn
F32 = jnp.float32
I32 = jnp.int32
BITS = 8
OUT = 96


def flat(y, core, zh, x, zl):
    return (((y * 2 + core) * 4 + zh) * 4 + x) * 2 + zl


def permutation(source_of):
    pairs = []
    for y in range(4):
        for core in range(2):
            for zh in range(4):
                for x in range(4):
                    for zl in range(2):
                        s = source_of(y, core, zh, x, zl)
                        if s is not None:
                            pairs.append((flat(*s), flat(y, core, zh, x, zl)))
    return pairs


def slots(zh, zl):
    return ((zh + zl) % 4, (zh + 3 + 3 * zl) % 4)


def z_near(y, core, zh, x, zl):
    return (y, core, (zh + 3) % 4, x, 1) if zl == 0 else (y, core, (zh + 1) % 4, x, 0)


def z_far(y, core, zh, x, zl):
    return None if zl == 0 else (y, core, (zh + 2) % 4, x, 0)


def y_out(y, core, zh, x, zl):
    a, b = slots(zh, zl)
    away = 1 if zl == 0 else 3
    if y == (a + away) % 4:
        return (a, core, zh, x, zl)
    if y == (b - away) % 4:
        return (b, core, zh, x, zl)
    return None


def y_swap(y, core, zh, x, zl):
    a, b = slots(zh, zl)
    away = 1 if zl == 0 else 3
    oa, ob = (a + away) % 4, (b - away) % 4
    return ({a: b, b: a, oa: ob, ob: oa}[y], core, zh, x, zl)


def unpack(words, dtype):
    n = words.shape[1]
    shifts = lax.broadcasted_iota(I32, (32, n), 0)
    rows = [
        jnp.right_shift(jnp.broadcast_to(words[i : i + 1, :], (32, n)), shifts) & 1
        for i in range(words.shape[0])
    ]
    return jnp.concatenate(rows, 0).astype(F32).astype(dtype)


def place():
    y, core = lax.axis_index("y"), lax.axis_index("core")
    zh, x, zl = lax.axis_index("zh"), lax.axis_index("x"), lax.axis_index("zl")
    return y, core, zh, x, zl


def planes(words, bits):
    return jnp.concatenate([jnp.right_shift(words, b) & 1 for b in bits], 0)


def count_kernel(idp, own, hub, r0, rp, rm, r2, yy, yc, out, keep, lhs, rhs, near, turned, res):
    y, core, zh, x, zl = place()
    row, col = 2 * y + core, 4 * zh + x
    groups = (lax.rem(zh + zl, 4), lax.rem(zh + 3 + 3 * zl, 4))
    sources = ((r0, 0), (rp, 1), (rm, 3), (r2, 2))
    ids = idp[...]
    q = (lax.broadcasted_iota(I32, (256, 16), 1) == ids // 768).astype(jnp.bfloat16)
    r = (lax.broadcasted_iota(I32, (256, 768), 1) == ids % 768).astype(jnp.bfloat16)
    outer = (((0,), (0,)), ((), ()))
    keep[...] = jnp.where(lax.dot_general(q, r, outer, preferred_element_type=F32) > 0.5, 0, -1)
    wordhot = (lax.broadcasted_iota(I32, (256, 48), 1) + 48 * row == ids // 32).astype(F32)
    bithot = (lax.broadcasted_iota(I32, (256, 32), 1) == ids % 32).astype(F32)
    light = 1.0 - lax.dot_general(
        wordhot.astype(jnp.bfloat16), bithot.astype(jnp.bfloat16), outer, preferred_element_type=F32
    )
    for n, (ref, rel) in enumerate(sources):
        xs = lax.rem(x + rel, 4)
        other = (xs // 2) != core
        for s in range(2):
            at = pl.multiple_of(48 * s + 24 * lax.rem(xs, 2), 8)
            words = jnp.where(other, yc[pl.ds(at, 24), :], yy[pl.ds(at, 24), :])
            base = (2 * n + s) * 768
            for part in range(3):
                rhs[base + 256 * part : base + 256 * part + 256, :] = unpack(
                    words[8 * part : 8 * part + 8, :], F8
                )
    keep_col = keep[pl.ds(col, 1), :]
    mine = own[...] & keep_col
    hub_col = planes(hub[...] & keep_col, range(32)).astype(F32)
    near[...] = hub_col.astype(F8)
    for side in range(2):
        xs = 2 * core + side
        words = jnp.zeros((8, 768), I32)
        for ref, rel in sources:
            for s in range(2):
                hit = (lax.rem(x + rel, 4) == xs) & (groups[s] == y)
                words = jnp.where(hit, ref[56 * s + 48 : 56 * s + 56, :], words)
        words = words & keep[pl.ds(2 * row + side, 1), :]
        turned[768 * side : 768 * side + 768, :] = jnp.concatenate([words] * 16, 0).T
    lane = lax.broadcasted_iota(I32, (48, 128), 1) // 8
    first = (zl == 0).astype(F32)
    once = (col == 0).astype(F32)
    tiles = 32 // BITS
    for t in range(tiles + 1):
        hubs = t == tiles
        size = 256 if hubs else 48 * BITS
        for n, (ref, rel) in enumerate(sources):
            xs = lax.rem(x + rel, 4)
            for s in range(2):
                lo, hi = (56 * s + 48, 56 * s + 56) if hubs else (56 * s, 56 * s + 48)
                words = ref[lo:hi, :] & keep[pl.ds(4 * groups[s] + xs, 1), :]
                bits = planes(words, range(32) if hubs else range(t * BITS, t * BITS + BITS))
                base = (2 * n + s) * 768
                lhs[t % 2, :size, base : base + 768] = bits.astype(F32).astype(F8)
        paths = jnp.dot(lhs[t % 2, :size, :], rhs[...], preferred_element_type=F32)
        if hubs:
            hub_tri = 0.5 * jnp.sum(paths * hub_col, axis=1, keepdims=True)
            hub_deg = first * jnp.sum(hub_col, axis=1, keepdims=True)
            spread = jnp.concatenate([hub_tri * bithot, hub_deg * bithot], 1)
            hub_part = lax.dot_general(
                wordhot,
                spread,
                outer,
                precision=lax.Precision.HIGHEST,
                preferred_element_type=F32,
            )
        else:
            edges = planes(mine, range(t * BITS, t * BITS + BITS)).astype(F32)
            reach = lax.dot_general(
                edges.astype(F8),
                near[...],
                (((1,), (1,)), ((), ())),
                preferred_element_type=F32,
            )
            for b in range(BITS):
                at = t * BITS + b
                rows = slice(48 * b, 48 * b + 48)
                words = turned[pl.ds(at, 48, stride=32), :]
                low = (jnp.right_shift(words, lane) & 1).astype(F32)
                high = (jnp.right_shift(words, lane + 16) & 1).astype(F32)
                closed = paths[rows, :] * edges[rows, :]
                with_hub = reach[rows, :128] * low + reach[rows, 128:] * high
                res[:, at : at + 1] = 0.5 * jnp.sum(closed, axis=1, keepdims=True) + jnp.sum(
                    with_hub, axis=1, keepdims=True
                )
                res[:, 32 + at : 33 + at] = first * jnp.sum(
                    edges[rows, :], axis=1, keepdims=True
                ) + once * jnp.sum(low + high, axis=1, keepdims=True)
    light = jnp.concatenate([light, light], 1)
    total = res[...] * light + hub_part
    out[...] = jnp.zeros_like(out)
    for c in range(16):
        for z in range(2):
            out[2 * c + z, 0:3, 0:64] = total[3 * c : 3 * c + 3, :]


def call(kernel, outs, scratch, args, flops):
    vmem = pl.BlockSpec(memory_space=pltpu.VMEM)
    return pl.pallas_call(
        kernel,
        out_shape=[jax.ShapeDtypeStruct(s, F32) for s in outs],
        in_specs=[vmem] * len(args),
        out_specs=[vmem] * len(outs),
        scratch_shapes=scratch,
        cost_estimate=pl.CostEstimate(flops=flops, bytes_accessed=1 << 20, transcendentals=0),
        compiler_params=pltpu.CompilerParams(vmem_limit_bytes=28 * 2**20),
    )(*args)


def body(light_bits, hub_bits, hub_ids):
    y, core, zh, x, zl = place()
    send = functools.partial(lax.ppermute, axis_name=AXES)
    even = zl == 0
    twin = lax.ppermute(hub_bits, "zl", [(0, 1), (1, 0)])
    hub = jnp.concatenate([jnp.where(even, hub_bits, twin), jnp.where(even, twin, hub_bits)], 0)
    block = jnp.concatenate([light_bits, hub], 0)
    near = send(block, perm=permutation(z_near))
    far = send(block, perm=permutation(z_far))
    group = jnp.concatenate([jnp.where(even, block, near), jnp.where(even, near, far)], 0)
    ring = [
        lax.ppermute(group, "x", [((d + r) % 4, d) for d in range(4)]) for r in (1, 3, 2)
    ]
    out = send(light_bits, perm=permutation(y_out))
    ga, gb = (zh + zl) % 4, (zh + 3 + 3 * zl) % 4
    root = (y == ga) | (y == gb)
    have = jnp.where(root, light_bits, out)
    got = send(have, perm=permutation(y_swap))
    first = (y == ga) | (y == (ga + 1 + 2 * zl) % 4)
    yy = jnp.concatenate([jnp.where(first, have, got), jnp.where(first, got, have)], 0)
    yc = lax.ppermute(yy, "core", [(0, 1), (1, 0)])
    planed = hub_ids.reshape(8, 32).T.reshape(256, 1)
    (table,) = call(
        count_kernel,
        [(32, 8, 128)],
        [
            pltpu.VMEM((16, 768), I32),
            pltpu.VMEM((2, 48 * BITS, 6144), F8),
            pltpu.VMEM((6144, 768), F8),
            pltpu.VMEM((256, 768), F8),
            pltpu.VMEM((1536, 128), I32),
            pltpu.VMEM((48, 64), F32),
        ],
        (planed, light_bits, hub, group, *ring, yy, yc),
        1 << 33,
    )
    everyone = lax.all_to_all(table, ("zh", "x", "zl"), 0, 0, tiled=True)
    total = jnp.sum(everyone, axis=0)
    return (total[:3, :32] / (1.0 + total[:3, 32:64])).reshape(OUT)


def solution(mesh):
    finer = Mesh(mesh.devices.reshape(SIZES), AXES)
    placed = (P(ROWS, COLS), P("zl", COLS), P())
    return jax.shard_map(
        body, mesh=finer, in_specs=placed, out_specs=P(ROWS + COLS), check_vma=False
    )
```

```python
import functools

import jax
import jax.numpy as jnp
from jax import lax
from jax.experimental import pallas as pl
from jax.experimental.pallas import tpu as pltpu
from jax.sharding import Mesh
from jax.sharding import PartitionSpec as P

AXES = ("y", "core", "zh", "x", "zl")
ROWS = ("y", "core")
COLS = ("zh", "x")
SIZES = (4, 2, 4, 4, 2)
F8 = jnp.float8_e4m3fn
F32 = jnp.float32
I32 = jnp.int32
BITS = 8
OUT = 96


def flat(y, core, zh, x, zl):
    return (((y * 2 + core) * 4 + zh) * 4 + x) * 2 + zl


def permutation(source_of):
    pairs = []
    for y in range(4):
        for core in range(2):
            for zh in range(4):
                for x in range(4):
                    for zl in range(2):
                        s = source_of(y, core, zh, x, zl)
                        if s is not None:
                            pairs.append((flat(*s), flat(y, core, zh, x, zl)))
    return pairs


def group_of(y, zh, zl):
    return y ^ (2 * (zh & 1) + zl)


def fetch(y, core, zh, x, zl):
    group = group_of(y, zh, zl)
    turn = y >> 1 if y in (0, 2) else int(group in (0, 3))
    return (y, core, group, x, turn ^ (zh >> 1))


def partner(y, core, zh, x, zl):
    return (y, core, zh ^ 1, x, zl)


def along_y(y, core, zh, x, zl):
    return (group_of(y, zh, zl), core, zh, x, zl)


def unpack(words, dtype):
    n = words.shape[1]
    shifts = lax.broadcasted_iota(I32, (32, n), 0)
    rows = [
        jnp.right_shift(jnp.broadcast_to(words[i : i + 1, :], (32, n)), shifts) & 1
        for i in range(words.shape[0])
    ]
    return jnp.concatenate(rows, 0).astype(F32).astype(dtype)


def place():
    y, core = lax.axis_index("y"), lax.axis_index("core")
    zh, x, zl = lax.axis_index("zh"), lax.axis_index("x"), lax.axis_index("zl")
    return y, core, zh, x, zl


def planes(words, bits):
    return jnp.concatenate([jnp.right_shift(words, b) & 1 for b in bits], 0)


def count_kernel(idp, pair, hubs, r0, rp, rm, r2, yy, yc, out, keep, lhs, rhs, near, turned, res):
    y, core, zh, x, zl = place()
    row = 2 * y + core
    part_of = 2 * lax.rem(zh, 2) + zl
    group = y ^ part_of
    sources = ((r0, 0), (rp, 1), (rm, 3), (r2, 2))
    ids = idp[...]
    q = (lax.broadcasted_iota(I32, (256, 16), 1) == ids // 768).astype(jnp.bfloat16)
    r = (lax.broadcasted_iota(I32, (256, 768), 1) == ids % 768).astype(jnp.bfloat16)
    outer = (((0,), (0,)), ((), ()))
    keep[...] = jnp.where(lax.dot_general(q, r, outer, preferred_element_type=F32) > 0.5, 0, -1)
    wordhot = (lax.broadcasted_iota(I32, (256, 48), 1) + 48 * row == ids // 32).astype(F32)
    bithot = (lax.broadcasted_iota(I32, (256, 32), 1) == ids % 32).astype(F32)
    light = 1.0 - lax.dot_general(
        wordhot.astype(jnp.bfloat16), bithot.astype(jnp.bfloat16), outer, preferred_element_type=F32
    )
    for n, (ref, rel) in enumerate(sources):
        xs = lax.rem(x + rel, 4)
        other = (xs // 2) != core
        for side in range(2):
            at = pl.multiple_of(48 * side + 24 * lax.rem(xs, 2), 8)
            words = jnp.where(other, yc[pl.ds(at, 24), :], yy[pl.ds(at, 24), :])
            for part in range(3):
                base = 768 * n + 256 * part
                rhs[base : base + 256, 768 * side : 768 * side + 768] = unpack(
                    words[8 * part : 8 * part + 8, :], F8
                )
    left = pl.ds(8 * (zh // 2) + x, 1)
    right = pl.ds(8 * (zh // 2) + 4 + x, 1)
    mine = jnp.concatenate(
        [pair[0:48, :] & keep[left, :], pair[48:96, :] & keep[right, :]], 1
    )
    hub_words = jnp.concatenate(
        [hubs[0:8, :] & keep[left, :], hubs[8:16, :] & keep[right, :]], 1
    )
    hub_col = planes(hub_words, range(32)).astype(F32)
    near[...] = hub_col.astype(F8)
    for side in range(2):
        xs = 2 * core + side
        words = jnp.zeros((8, 768), I32)
        for ref, rel in sources:
            hit = (lax.rem(x + rel, 4) == xs) & (group == y)
            words = jnp.where(hit, ref[48:56, :], words)
        words = words & keep[pl.ds(2 * row + side, 1), :]
        turned[768 * side : 768 * side + 768, :] = jnp.concatenate([words] * 16, 0).T
    lane = lax.broadcasted_iota(I32, (48, 128), 1) // 8
    first = (part_of == 0).astype(F32)
    once = ((x == 0) & (zh < 2)).astype(F32)
    tiles = 32 // BITS
    for t in range(tiles + 1):
        extra = t == tiles
        size = 256 if extra else 48 * BITS
        for n, (ref, rel) in enumerate(sources):
            lo, hi = (48, 56) if extra else (0, 48)
            words = ref[lo:hi, :] & keep[pl.ds(4 * group + lax.rem(x + rel, 4), 1), :]
            bits = planes(words, range(32) if extra else range(t * BITS, t * BITS + BITS))
            lhs[t % 2, :size, 768 * n : 768 * n + 768] = bits.astype(F32).astype(F8)
        paths = jnp.dot(lhs[t % 2, :size, :], rhs[...], preferred_element_type=F32)
        if extra:
            hub_tri = 0.5 * jnp.sum(paths * hub_col, axis=1, keepdims=True)
            hub_deg = first * jnp.sum(hub_col, axis=1, keepdims=True)
            spread = jnp.concatenate([hub_tri * bithot, hub_deg * bithot], 1)
            hub_part = lax.dot_general(
                wordhot,
                spread,
                outer,
                precision=lax.Precision.HIGHEST,
                preferred_element_type=F32,
            )
        else:
            edges = planes(mine, range(t * BITS, t * BITS + BITS)).astype(F32)
            reach = lax.dot_general(
                edges.astype(F8),
                near[...],
                (((1,), (1,)), ((), ())),
                preferred_element_type=F32,
            )
            for b in range(BITS):
                at = t * BITS + b
                rows = slice(48 * b, 48 * b + 48)
                words = turned[pl.ds(at, 48, stride=32), :]
                low = (jnp.right_shift(words, lane) & 1).astype(F32)
                high = (jnp.right_shift(words, lane + 16) & 1).astype(F32)
                closed = paths[rows, :] * edges[rows, :]
                with_hub = reach[rows, :128] * low + reach[rows, 128:] * high
                res[:, at : at + 1] = 0.5 * jnp.sum(closed, axis=1, keepdims=True) + jnp.sum(
                    with_hub, axis=1, keepdims=True
                )
                res[:, 32 + at : 33 + at] = first * jnp.sum(
                    edges[rows, :], axis=1, keepdims=True
                ) + once * jnp.sum(low + high, axis=1, keepdims=True)
    light = jnp.concatenate([light, light], 1)
    total = res[...] * light + hub_part
    for c in range(16):
        line = jnp.concatenate(
            [total[3 * c + k : 3 * c + k + 1, 0:32] for k in range(3)]
            + [jnp.zeros((1, 32), F32)]
            + [total[3 * c + k : 3 * c + k + 1, 32:64] for k in range(3)]
            + [jnp.zeros((1, 32), F32)],
            1,
        )
        out[2 * c : 2 * c + 1, :] = line
        out[2 * c + 1 : 2 * c + 2, :] = line


def call(kernel, outs, scratch, args, flops):
    vmem = pl.BlockSpec(memory_space=pltpu.VMEM)
    return pl.pallas_call(
        kernel,
        out_shape=[jax.ShapeDtypeStruct(s, F32) for s in outs],
        in_specs=[vmem] * len(args),
        out_specs=[vmem] * len(outs),
        scratch_shapes=scratch,
        cost_estimate=pl.CostEstimate(flops=flops, bytes_accessed=1 << 20, transcendentals=0),
        compiler_params=pltpu.CompilerParams(vmem_limit_bytes=28 * 2**20),
    )(*args)


def clustering(light_bits, hub_bits, hub_ids):
    _, _, zh, _, zl = place()
    send = functools.partial(lax.ppermute, axis_name=AXES)
    even = zl == 0
    twin = lax.ppermute(hub_bits, "zl", [(0, 1), (1, 0)])
    block = jnp.concatenate(
        [light_bits, jnp.where(even, hub_bits, twin), jnp.where(even, twin, hub_bits)], 0
    )
    rows = send(block, perm=permutation(fetch))
    beside = send(block, perm=permutation(partner))
    ring = []
    for r in (1, 3, 2):
        ring.append(lax.ppermute(rows, "x", [((d + r) % 4, d) for d in range(4)]))
    lead = zh % 2 == 0
    left = jnp.where(lead, block, beside)
    right = jnp.where(lead, beside, block)
    pair = jnp.concatenate([left[:48], right[:48]], 0)
    hubs = jnp.concatenate([left[48:], right[48:]], 0)
    yy = send(pair, perm=permutation(along_y))
    yc = lax.ppermute(yy, "core", [(0, 1), (1, 0)])
    planed = hub_ids.reshape(8, 32).T.reshape(256, 1)
    (table,) = call(
        count_kernel,
        [(32, 256)],
        [
            pltpu.VMEM((16, 768), I32),
            pltpu.VMEM((2, 48 * BITS, 3072), F8),
            pltpu.VMEM((3072, 1536), F8),
            pltpu.VMEM((256, 1536), F8),
            pltpu.VMEM((1536, 128), I32),
            pltpu.VMEM((48, 64), F32),
        ],
        (planed, pair, hubs, rows, *ring, yy, yc),
        1 << 33,
    )
    everyone = lax.all_to_all(table, ("zh", "x", "zl"), 0, 0, tiled=True)
    total = jnp.sum(everyone, axis=0)
    return total[:OUT] / (1.0 + total[128 : 128 + OUT])


def solution(mesh):
    finer = Mesh(mesh.devices.reshape(SIZES), AXES)
    placed = (P(ROWS, COLS), P("zl", COLS), P())
    return jax.shard_map(
        clustering, mesh=finer, in_specs=placed, out_specs=P(ROWS + COLS), check_vma=False
    )
```

```python
import jax
import jax.numpy as jnp
from jax import lax
from jax.experimental import pallas as pl
from jax.experimental.pallas import tpu as pltpu
from jax.sharding import Mesh
from jax.sharding import PartitionSpec as P

AXES = ("y", "core", "zh", "x", "zl")
ROWS = ("y", "core")
COLS = ("zh", "x")
SIZES = (4, 2, 4, 4, 2)
F8 = jnp.float8_e4m3fn
F32 = jnp.float32
I32 = jnp.int32
OUT = 96


def flat(y, core, zh, x, zl):
    return (((y * 2 + core) * 4 + zh) * 4 + x) * 2 + zl


def permutation(source_of):
    pairs = []
    for y in range(4):
        for core in range(2):
            for zh in range(4):
                for x in range(4):
                    for zl in range(2):
                        s = source_of(y, core, zh, x, zl)
                        if s is not None:
                            pairs.append((flat(*s), flat(y, core, zh, x, zl)))
    return pairs


FETCH = ((0, 1, 0, 1), (1, 0, 0, 1), (1, 0, 1, 0), (1, 0, 0, 1))


def group_of(y, z):
    return (-(y + z)) & 3


def fetch(y, core, zh, x, zl):
    z = 2 * zh + zl
    group = group_of(y, z)
    return (y, core, group, x, FETCH[(-y) & 3][group] ^ (z >> 2))


def partner(y, core, zh, x, zl):
    return (y, core, (zh + 1) % 4, x, 0) if zl == 1 else (y, core, (zh + 3) % 4, x, 1)


def along_y(y, core, zh, x, zl):
    return (group_of(y, 2 * zh + zl), core, zh, x, zl)


def unpack(words, dtype):
    n = words.shape[1]
    shifts = lax.broadcasted_iota(I32, (32, n), 0)
    rows = [
        jnp.right_shift(jnp.broadcast_to(words[i : i + 1, :], (32, n)), shifts) & 1
        for i in range(words.shape[0])
    ]
    return jnp.concatenate(rows, 0).astype(F32).astype(dtype)


def place():
    y, core = lax.axis_index("y"), lax.axis_index("core")
    zh, x, zl = lax.axis_index("zh"), lax.axis_index("x"), lax.axis_index("zl")
    return y, core, zh, x, zl


def planes(words, bits):
    return jnp.concatenate([jnp.right_shift(words, b) & 1 for b in bits], 0)


def scaled(words, bits):
    return jnp.concatenate(
        [jnp.right_shift(words, b - b % 8) & (1 << (b % 8)) for b in bits], 0
    )


OUTER = (((0,), (0,)), ((), ()))


def left_kernel(idp, r0, rp, rm, r2, lhs, keep):
    y, _, zh, x, zl = place()
    group = (16 - y - 2 * zh - zl) & 3
    ids = idp[...]
    q = (lax.broadcasted_iota(I32, (256, 16), 1) == ids // 768).astype(jnp.bfloat16)
    r = (lax.broadcasted_iota(I32, (256, 768), 1) == ids % 768).astype(jnp.bfloat16)
    keep[...] = jnp.where(lax.dot_general(q, r, OUTER, preferred_element_type=F32) > 0.5, 0, -1)
    for n, (ref, rel) in enumerate(((r0, 0), (rp, 1), (rm, 3), (r2, 2))):
        words = ref[...] & keep[pl.ds(4 * group + lax.rem(x + rel, 4), 1), :]
        at = slice(768 * n, 768 * n + 768)
        for t in range(4):
            bits = scaled(words[:48], range(8 * t, 8 * t + 8))
            lhs[384 * t : 384 * t + 384, at] = bits.astype(F32).astype(F8)
        lhs[1536:1792, at] = scaled(words[48:], range(32)).astype(F32).astype(F8)


def count_kernel(idp, keep, pair, hubs, r0, rp, rm, r2, yy, yc, lhs, out, rhs, near, turned, res):
    y, core, zh, x, zl = place()
    row = 2 * y + core
    z = 2 * zh + zl
    group = (16 - y - z) & 3
    sources = ((r0, 0), (rp, 1), (rm, 3), (r2, 2))
    ids = idp[...]
    wordhot = (lax.broadcasted_iota(I32, (256, 48), 1) + 48 * row == ids // 32).astype(F32)
    bithot = (lax.broadcasted_iota(I32, (256, 32), 1) == ids % 32).astype(F32)
    light = 1.0 - lax.dot_general(
        wordhot.astype(jnp.bfloat16), bithot.astype(jnp.bfloat16), OUTER, preferred_element_type=F32
    )
    for n, (ref, rel) in enumerate(sources):
        xs = lax.rem(x + rel, 4)
        other = (xs // 2) != core
        for side in range(2):
            at = pl.multiple_of(48 * side + 24 * lax.rem(xs, 2), 8)
            words = jnp.where(other, yc[pl.ds(at, 24), :], yy[pl.ds(at, 24), :])
            for part in range(3):
                base = 768 * n + 256 * part
                rhs[base : base + 256, 768 * side : 768 * side + 768] = unpack(
                    words[8 * part : 8 * part + 8, :], F8
                )
    zhl = (zh + 3 + zl) & 3
    left = pl.ds(4 * zhl + x, 1)
    right = pl.ds(4 * ((zhl + 1) & 3) + x, 1)
    mine = jnp.concatenate(
        [pair[0:48, :] & keep[left, :], pair[48:96, :] & keep[right, :]], 1
    )
    hub_words = jnp.concatenate(
        [hubs[0:8, :] & keep[left, :], hubs[8:16, :] & keep[right, :]], 1
    )
    hub_col = planes(hub_words, range(32)).astype(F32)
    near[...] = hub_col.astype(F8)
    for side in range(2):
        xs = 2 * core + side
        words = jnp.zeros((8, 768), I32)
        for ref, rel in sources:
            hit = (lax.rem(x + rel, 4) == xs) & (group == y)
            words = jnp.where(hit, ref[48:56, :], words)
        words = words & keep[pl.ds(2 * row + side, 1), :]
        turned[768 * side : 768 * side + 768, :] = jnp.concatenate([words] * 16, 0).T
    lane = lax.broadcasted_iota(I32, (48, 128), 1) // 8
    first = (zl == 0).astype(F32)
    once = ((x == 0) & (z == ((16 - 2 * y) & 3))).astype(F32)
    for t in range(4):
        paths = jnp.dot(
            lhs[384 * t : 384 * t + 384, :], rhs[...], preferred_element_type=F32
        )
        edges = planes(mine, range(8 * t, 8 * t + 8)).astype(F32)
        reach = lax.dot_general(
            edges.astype(F8), near[...], (((1,), (1,)), ((), ())), preferred_element_type=F32
        )
        for b in range(8):
            at = 8 * t + b
            rows = slice(48 * b, 48 * b + 48)
            words = turned[pl.ds(at, 48, stride=32), :]
            low = (jnp.right_shift(words, lane) & 1).astype(F32)
            high = (jnp.right_shift(words, lane + 16) & 1).astype(F32)
            closed = paths[rows, :] * edges[rows, :]
            with_hub = reach[rows, :128] * low + reach[rows, 128:] * high
            res[:, at : at + 1] = (0.5 / (1 << b)) * jnp.sum(
                closed, axis=1, keepdims=True
            ) + jnp.sum(with_hub, axis=1, keepdims=True)
            res[:, 32 + at : 33 + at] = first * jnp.sum(
                edges[rows, 768:], axis=1, keepdims=True
            ) + once * jnp.sum(low + high, axis=1, keepdims=True)
    paths = jnp.dot(lhs[1536:1792, :], rhs[...], preferred_element_type=F32)
    bit = (lax.broadcasted_iota(I32, (256, 1), 0) // 8) & 7
    unscale = jnp.right_shift(128, bit).astype(F32) * (0.5 / 128)
    hub_tri = unscale * jnp.sum(paths * hub_col, axis=1, keepdims=True)
    hub_deg = first * jnp.sum(hub_col[:, 768:], axis=1, keepdims=True)
    hub_part = lax.dot_general(
        wordhot,
        jnp.concatenate([hub_tri * bithot, hub_deg * bithot], 1),
        OUTER,
        precision=lax.Precision.HIGHEST,
        preferred_element_type=F32,
    )
    total = res[...] * jnp.concatenate([light, light], 1) + hub_part
    for c in range(16):
        line = jnp.concatenate(
            [total[3 * c + k : 3 * c + k + 1, 0:32] for k in range(3)]
            + [jnp.zeros((1, 32), F32)]
            + [total[3 * c + k : 3 * c + k + 1, 32:64] for k in range(3)]
            + [jnp.zeros((1, 32), F32)],
            1,
        )
        out[2 * c : 2 * c + 1, :] = line
        out[2 * c + 1 : 2 * c + 2, :] = line


def call(kernel, outs, scratch, args, flops, limit):
    vmem = pl.BlockSpec(memory_space=pltpu.VMEM)
    return pl.pallas_call(
        kernel,
        out_shape=[jax.ShapeDtypeStruct(*o) for o in outs],
        in_specs=[vmem] * len(args),
        out_specs=[vmem] * len(outs),
        scratch_shapes=scratch,
        cost_estimate=pl.CostEstimate(flops=flops, bytes_accessed=1 << 20, transcendentals=0),
        compiler_params=pltpu.CompilerParams(vmem_limit_bytes=limit * 2**20),
    )(*args)


def clustering(light_bits, hub_bits, hub_ids):
    _, _, _, _, zl = place()

    def send(value, source):
        return lax.ppermute(value, AXES, perm=permutation(source))

    rows = send(light_bits, fetch)
    beside = send(light_bits, partner)
    twin = send(hub_bits, lambda y, core, zh, x, zl: (y, core, zh, x, zl ^ 1))
    even = zl == 0
    hub = jnp.concatenate([jnp.where(even, hub_bits, twin), jnp.where(even, twin, hub_bits)], 0)
    hub_rows = send(hub, fetch)
    hub_beside = send(hub, partner)
    rows = jnp.concatenate([rows, hub_rows], 0)
    ring = [
        send(rows, lambda y, core, zh, x, zl, r=r: (y, core, zh, (x + r) % 4, zl))
        for r in (1, 3, 2)
    ]
    pair = jnp.concatenate(
        [jnp.where(even, beside, light_bits), jnp.where(even, light_bits, beside)], 0
    )
    hubs = jnp.concatenate([jnp.where(even, hub_beside, hub), jnp.where(even, hub, hub_beside)], 0)
    yy = send(pair, along_y)
    yc = send(yy, lambda y, core, zh, x, zl: (y, core ^ 1, zh, x, zl))
    planed = hub_ids.reshape(8, 32).T.reshape(256, 1)
    lhs, keep = call(
        left_kernel,
        [((1792, 3072), F8), ((16, 768), I32)],
        [],
        (planed, rows, *ring),
        1 << 30,
        12,
    )
    (table,) = call(
        count_kernel,
        [((32, 256), F32)],
        [
            pltpu.VMEM((3072, 1536), F8),
            pltpu.VMEM((256, 1536), F8),
            pltpu.VMEM((1536, 128), I32),
            pltpu.VMEM((48, 64), F32),
        ],
        (planed, keep, pair, hubs, rows, *ring, yy, yc, lhs),
        1 << 33,
        26,
    )
    everyone = lax.all_to_all(table, ("zh", "x", "zl"), 0, 0, tiled=True)
    total = jnp.sum(everyone, axis=0)
    return total[:OUT] / (1.0 + total[128 : 128 + OUT])


def solution(mesh):
    finer = Mesh(mesh.devices.reshape(SIZES), AXES)
    placed = (P(ROWS, COLS), P("zl", COLS), P())
    return jax.shard_map(
        clustering, mesh=finer, in_specs=placed, out_specs=P(ROWS + COLS), check_vma=False
    )
```

```python
import jax
import jax.numpy as jnp
from jax import lax
from jax.experimental import pallas as pl
from jax.experimental.pallas import tpu as pltpu
from jax.sharding import Mesh
from jax.sharding import PartitionSpec as P

AXES = ("y", "core", "zh", "x", "zl")
ROWS = ("y", "core")
COLS = ("zh", "x")
SIZES = (4, 2, 4, 4, 2)
F8 = jnp.float8_e4m3fn
F32 = jnp.float32
I32 = jnp.int32
OUT = 96


def flat(y, core, zh, x, zl):
    return (((y * 2 + core) * 4 + zh) * 4 + x) * 2 + zl


def permutation(source_of):
    pairs = []
    for y in range(4):
        for core in range(2):
            for zh in range(4):
                for x in range(4):
                    for zl in range(2):
                        s = source_of(y, core, zh, x, zl)
                        if s is not None:
                            pairs.append((flat(*s), flat(y, core, zh, x, zl)))
    return pairs


FETCH = ((0, 1, 0, 1), (1, 0, 0, 1), (1, 0, 1, 0), (1, 0, 0, 1))


def group_of(y, z):
    return (-(y + z)) & 3


def fetch(y, core, zh, x, zl):
    z = 2 * zh + zl
    group = group_of(y, z)
    return (y, core, group, x, FETCH[(-y) & 3][group] ^ (z >> 2))


def partner(y, core, zh, x, zl):
    return (y, core, (zh + 1) % 4, x, 0) if zl == 1 else (y, core, (zh + 3) % 4, x, 1)


def along_y(y, core, zh, x, zl):
    return (group_of(y, 2 * zh + zl), core, zh, x, zl)


def unpack(words, dtype):
    n = words.shape[1]
    shifts = lax.broadcasted_iota(I32, (32, n), 0)
    rows = [
        jnp.right_shift(jnp.broadcast_to(words[i : i + 1, :], (32, n)), shifts) & 1
        for i in range(words.shape[0])
    ]
    return jnp.concatenate(rows, 0).astype(F32).astype(dtype)


def place():
    y, core = lax.axis_index("y"), lax.axis_index("core")
    zh, x, zl = lax.axis_index("zh"), lax.axis_index("x"), lax.axis_index("zl")
    return y, core, zh, x, zl


def planes(words, bits):
    return jnp.concatenate([jnp.right_shift(words, b) & 1 for b in bits], 0)


def scaled(words, bits):
    return jnp.concatenate(
        [jnp.right_shift(words, b - b % 8) & (1 << (b % 8)) for b in bits], 0
    )


OUTER = (((0,), (0,)), ((), ()))


def left_kernel(idp, r0, rp, rm, r2, lhs, keep):
    y, _, zh, x, zl = place()
    group = (16 - y - 2 * zh - zl) & 3
    ids = idp[...]
    q = (lax.broadcasted_iota(I32, (256, 16), 1) == ids // 768).astype(jnp.bfloat16)
    r = (lax.broadcasted_iota(I32, (256, 768), 1) == ids % 768).astype(jnp.bfloat16)
    keep[...] = jnp.where(lax.dot_general(q, r, OUTER, preferred_element_type=F32) > 0.5, 0, -1)
    for n, (ref, rel) in enumerate(((r0, 0), (rp, 1), (rm, 3), (r2, 2))):
        words = ref[...] & keep[pl.ds(4 * group + lax.rem(x + rel, 4), 1), :]
        at = slice(768 * n, 768 * n + 768)
        for t in range(4):
            bits = scaled(words[:48], range(8 * t, 8 * t + 8))
            lhs[384 * t : 384 * t + 384, at] = bits.astype(F32).astype(F8)
        lhs[1536:1792, at] = scaled(words[48:], range(32)).astype(F32).astype(F8)


def right_kernel(yy, yc, rhs):
    _, core, _, x, _ = place()
    for n, rel in enumerate((0, 1, 3, 2)):
        xs = lax.rem(x + rel, 4)
        other = (xs // 2) != core
        for side in range(2):
            at = pl.multiple_of(48 * side + 24 * lax.rem(xs, 2), 8)
            words = jnp.where(other, yc[pl.ds(at, 24), :], yy[pl.ds(at, 24), :])
            for part in range(3):
                base = 768 * n + 256 * part
                rhs[base : base + 256, 768 * side : 768 * side + 768] = unpack(
                    words[8 * part : 8 * part + 8, :], F8
                )


def count_kernel(idp, keep, pair, hubs, r0, rp, rm, r2, lhs, rhs, out, near, turned, res):
    y, core, zh, x, zl = place()
    row = 2 * y + core
    z = 2 * zh + zl
    group = (16 - y - z) & 3
    sources = ((r0, 0), (rp, 1), (rm, 3), (r2, 2))
    ids = idp[...]
    wordhot = (lax.broadcasted_iota(I32, (256, 48), 1) + 48 * row == ids // 32).astype(F32)
    bithot = (lax.broadcasted_iota(I32, (256, 32), 1) == ids % 32).astype(F32)
    light = 1.0 - lax.dot_general(
        wordhot.astype(jnp.bfloat16), bithot.astype(jnp.bfloat16), OUTER, preferred_element_type=F32
    )
    own = pl.ds(4 * zh + x, 1)
    side = pl.ds(4 * ((zh + 3 + 2 * zl) & 3) + x, 1)
    mine = jnp.concatenate([pair[0:48, :] & keep[own, :], pair[48:96, :] & keep[side, :]], 1)
    hub_words = jnp.concatenate(
        [hubs[0:8, :] & keep[own, :], hubs[8:16, :] & keep[side, :]], 1
    )
    hub_col = planes(hub_words, range(32)).astype(F32)
    near[...] = hub_col.astype(F8)
    for side in range(2):
        xs = 2 * core + side
        words = jnp.zeros((8, 768), I32)
        for ref, rel in sources:
            hit = (lax.rem(x + rel, 4) == xs) & (group == y)
            words = jnp.where(hit, ref[48:56, :], words)
        words = words & keep[pl.ds(2 * row + side, 1), :]
        turned[768 * side : 768 * side + 768, :] = jnp.concatenate([words] * 16, 0).T
    lane = lax.broadcasted_iota(I32, (48, 128), 1) // 8
    first = (zl == 0).astype(F32)
    once = ((x == 0) & (z == ((16 - 2 * y) & 3))).astype(F32)
    for t in range(4):
        paths = jnp.dot(
            lhs[384 * t : 384 * t + 384, :], rhs[...], preferred_element_type=F32
        )
        edges = planes(mine, range(8 * t, 8 * t + 8)).astype(F32)
        reach = lax.dot_general(
            edges.astype(F8), near[...], (((1,), (1,)), ((), ())), preferred_element_type=F32
        )
        for b in range(8):
            at = 8 * t + b
            rows = slice(48 * b, 48 * b + 48)
            words = turned[pl.ds(at, 48, stride=32), :]
            low = (jnp.right_shift(words, lane) & 1).astype(F32)
            high = (jnp.right_shift(words, lane + 16) & 1).astype(F32)
            closed = paths[rows, :] * edges[rows, :]
            with_hub = reach[rows, :128] * low + reach[rows, 128:] * high
            res[:, at : at + 1] = (0.5 / (1 << b)) * jnp.sum(
                closed, axis=1, keepdims=True
            ) + jnp.sum(with_hub, axis=1, keepdims=True)
            res[:, 32 + at : 33 + at] = first * jnp.sum(
                edges[rows, :768], axis=1, keepdims=True
            ) + once * jnp.sum(low + high, axis=1, keepdims=True)
    paths = jnp.dot(lhs[1536:1792, :], rhs[...], preferred_element_type=F32)
    bit = (lax.broadcasted_iota(I32, (256, 1), 0) // 8) & 7
    unscale = jnp.right_shift(128, bit).astype(F32) * (0.5 / 128)
    hub_tri = unscale * jnp.sum(paths * hub_col, axis=1, keepdims=True)
    hub_deg = first * jnp.sum(hub_col[:, :768], axis=1, keepdims=True)
    hub_part = lax.dot_general(
        wordhot,
        jnp.concatenate([hub_tri * bithot, hub_deg * bithot], 1),
        OUTER,
        precision=lax.Precision.HIGHEST,
        preferred_element_type=F32,
    )
    total = res[...] * jnp.concatenate([light, light], 1) + hub_part
    for c in range(16):
        line = jnp.concatenate(
            [total[3 * c + k : 3 * c + k + 1, 0:32] for k in range(3)]
            + [jnp.zeros((1, 32), F32)]
            + [total[3 * c + k : 3 * c + k + 1, 32:64] for k in range(3)]
            + [jnp.zeros((1, 32), F32)],
            1,
        )
        out[2 * c : 2 * c + 1, :] = line
        out[2 * c + 1 : 2 * c + 2, :] = line


def call(kernel, outs, scratch, args, flops, limit):
    vmem = pl.BlockSpec(memory_space=pltpu.VMEM)
    return pl.pallas_call(
        kernel,
        out_shape=[jax.ShapeDtypeStruct(*o) for o in outs],
        in_specs=[vmem] * len(args),
        out_specs=[vmem] * len(outs),
        scratch_shapes=scratch,
        cost_estimate=pl.CostEstimate(flops=flops, bytes_accessed=1 << 20, transcendentals=0),
        compiler_params=pltpu.CompilerParams(vmem_limit_bytes=limit * 2**20),
    )(*args)


def clustering(light_bits, hub_bits, hub_ids):
    _, _, _, _, zl = place()

    def send(value, source):
        return lax.ppermute(value, AXES, perm=permutation(source))

    rows = send(light_bits, fetch)
    beside = send(light_bits, partner)
    twin = send(hub_bits, lambda y, core, zh, x, zl: (y, core, zh, x, zl ^ 1))
    even = zl == 0
    hub = jnp.concatenate([jnp.where(even, hub_bits, twin), jnp.where(even, twin, hub_bits)], 0)
    hub_rows = send(hub, fetch)
    hub_beside = send(hub, partner)
    rows = jnp.concatenate([rows, hub_rows], 0)
    ring = [
        send(rows, lambda y, core, zh, x, zl, r=r: (y, core, zh, (x + r) % 4, zl))
        for r in (1, 3, 2)
    ]
    pair = jnp.concatenate([light_bits, beside], 0)
    hubs = jnp.concatenate([hub, hub_beside], 0)
    yy = send(pair, along_y)
    yc = send(yy, lambda y, core, zh, x, zl: (y, core ^ 1, zh, x, zl))
    planed = hub_ids.reshape(8, 32).T.reshape(256, 1)
    (rhs,) = call(right_kernel, [((3072, 1536), F8)], [], (yy, yc), 1 << 30, 8)
    lhs, keep = call(
        left_kernel,
        [((1792, 3072), F8), ((16, 768), I32)],
        [],
        (planed, rows, *ring),
        1 << 30,
        12,
    )
    (table,) = call(
        count_kernel,
        [((32, 256), F32)],
        [
            pltpu.VMEM((256, 1536), F8),
            pltpu.VMEM((1536, 128), I32),
            pltpu.VMEM((48, 64), F32),
        ],
        (planed, keep, pair, hubs, rows, *ring, lhs, rhs),
        1 << 33,
        24,
    )
    everyone = lax.all_to_all(table, ("zh", "x", "zl"), 0, 0, tiled=True)
    total = jnp.sum(everyone, axis=0)
    return total[:OUT] / (1.0 + total[128 : 128 + OUT])


def solution(mesh):
    finer = Mesh(mesh.devices.reshape(SIZES), AXES)
    placed = (P(ROWS, COLS), P("zl", COLS), P())
    return jax.shard_map(
        clustering, mesh=finer, in_specs=placed, out_specs=P(ROWS + COLS), check_vma=False
    )
```

```python
import jax
import jax.numpy as jnp
from jax import lax
from jax.experimental import pallas as pl
from jax.experimental.pallas import tpu as pltpu
from jax.sharding import Mesh
from jax.sharding import PartitionSpec as P

AXES = ("y", "core", "zh", "x", "zl")
ROWS = ("y", "core")
COLS = ("zh", "x")
SIZES = (4, 2, 4, 4, 2)
F8 = jnp.float8_e4m3fn
F32 = jnp.float32
I32 = jnp.int32
I8 = jnp.int8
BF16 = jnp.bfloat16
OUT = 96


def flat(y, core, zh, x, zl):
    return (((y * 2 + core) * 4 + zh) * 4 + x) * 2 + zl


def permutation(source_of):
    pairs = []
    for y in range(4):
        for core in range(2):
            for zh in range(4):
                for x in range(4):
                    for zl in range(2):
                        s = source_of(y, core, zh, x, zl)
                        if s is not None:
                            pairs.append((flat(*s), flat(y, core, zh, x, zl)))
    return pairs


FETCH = ((0, 1, 0, 1), (1, 0, 0, 1), (1, 0, 1, 0), (1, 0, 0, 1))


def group_of(y, z):
    return (-(y + z)) & 3


def fetch(y, core, zh, x, zl):
    z = 2 * zh + zl
    group = group_of(y, z)
    return (y, core, group, x, FETCH[(-y) & 3][group] ^ (z >> 2))


def partner(y, core, zh, x, zl):
    return (y, core, (zh + 1) % 4, x, 0) if zl == 1 else (y, core, (zh + 3) % 4, x, 1)


def along_y(y, core, zh, x, zl):
    return (group_of(y, 2 * zh + zl), core, zh, x, zl)


def unpack(words):
    n = words.shape[1]
    shifts = lax.broadcasted_iota(I32, (32, n), 0)
    rows = [
        jnp.right_shift(jnp.broadcast_to(words[i : i + 1, :], (32, n)), shifts)
        for i in range(words.shape[0])
    ]
    bits = jnp.concatenate(rows, 0).astype(I8) & I8(1)
    return bits.astype(BF16).astype(F8)


def place():
    y, core = lax.axis_index("y"), lax.axis_index("core")
    zh, x, zl = lax.axis_index("zh"), lax.axis_index("x"), lax.axis_index("zl")
    return y, core, zh, x, zl


def planes(words, bits):
    return jnp.concatenate([jnp.right_shift(words, b) & 1 for b in bits], 0)


def octets(words, at):
    return jnp.concatenate([jnp.right_shift(words, a) for a in at], 0).astype(I8)


def plane(bytes8, b):
    return (bytes8 & I8(SCALE[b])).astype(BF16).astype(F8)


SCALE = (1, 2, 4, 8, 16, 32, 64, -128)
OUTER = (((0,), (0,)), ((), ()))


def right_kernel(yy, yc, rhs):
    _, core, _, x, _ = place()
    for n, rel in enumerate((0, 1, 3, 2)):
        xs = lax.rem(x + rel, 4)
        other = (xs // 2) != core
        for side in range(2):
            at = pl.multiple_of(48 * side + 24 * lax.rem(xs, 2), 8)
            words = jnp.where(other, yc[pl.ds(at, 24), :], yy[pl.ds(at, 24), :])
            for part in range(3):
                base = 768 * n + 256 * part
                rhs[base : base + 256, 768 * side : 768 * side + 768] = unpack(
                    words[8 * part : 8 * part + 8, :]
                )


def count_kernel(idp, pair, hubs, r0, rp, rm, r2, rhs, out, keep, lhs, near, turned, res):
    y, core, zh, x, zl = place()
    row = 2 * y + core
    z = 2 * zh + zl
    group = (16 - y - z) & 3
    sources = ((r0, 0), (rp, 1), (rm, 3), (r2, 2))
    ids = idp[...]
    q = (lax.broadcasted_iota(I32, (256, 16), 1) == ids // 768).astype(BF16)
    r = (lax.broadcasted_iota(I32, (256, 768), 1) == ids % 768).astype(BF16)
    keep[...] = jnp.where(lax.dot_general(q, r, OUTER, preferred_element_type=F32) > 0.5, 0, -1)
    wordhot = (lax.broadcasted_iota(I32, (256, 48), 1) + 48 * row == ids // 32).astype(F32)
    bithot = (lax.broadcasted_iota(I32, (256, 32), 1) == ids % 32).astype(F32)
    light = 1.0 - lax.dot_general(
        wordhot.astype(BF16), bithot.astype(BF16), OUTER, preferred_element_type=F32
    )
    own = pl.ds(4 * zh + x, 1)
    side = pl.ds(4 * ((zh + 3 + 2 * zl) & 3) + x, 1)
    mine = jnp.concatenate([pair[0:48, :] & keep[own, :], pair[48:96, :] & keep[side, :]], 1)
    hub_words = jnp.concatenate(
        [hubs[0:8, :] & keep[own, :], hubs[8:16, :] & keep[side, :]], 1
    )
    hub_col = planes(hub_words, range(32)).astype(F32)
    near[...] = hub_col.astype(F8)
    for side in range(2):
        xs = 2 * core + side
        words = jnp.zeros((8, 768), I32)
        for ref, rel in sources:
            hit = (lax.rem(x + rel, 4) == xs) & (group == y)
            words = jnp.where(hit, ref[48:56, :], words)
        words = words & keep[pl.ds(2 * row + side, 1), :]
        turned[768 * side : 768 * side + 768, :] = jnp.concatenate([words] * 16, 0).T
    lane = lax.broadcasted_iota(I32, (48, 128), 1) // 8
    first = (zl == 0).astype(F32)
    once = ((x == 0) & (z == ((16 - 2 * y) & 3))).astype(F32)

    def masked(ref, rel, rows):
        return ref[rows, :] & keep[pl.ds(4 * group + lax.rem(x + rel, 4), 1), :]

    def fill(tile):
        half, quarter = tile // 2, tile % 2
        for n, (ref, rel) in enumerate(sources):
            words = masked(ref, rel, slice(0, 48))
            both = octets(words, (16 * half, 16 * half + 8))
            for b in range(4):
                lhs[tile % 2, 96 * b : 96 * b + 96, 768 * n : 768 * n + 768] = plane(
                    both, 4 * quarter + b
                )

    fill(0)
    for tile in range(4):
        half, quarter = tile // 2, tile % 2
        paths = jnp.dot(lhs[tile % 2], rhs[...], preferred_element_type=F32)
        if tile < 3:
            fill(tile + 1)
        else:
            for n, (ref, rel) in enumerate(sources):
                words = octets(masked(ref, rel, slice(48, 56)), (0, 8, 16, 24))
                for b in range(8):
                    lhs[0, 32 * b : 32 * b + 32, 768 * n : 768 * n + 768] = plane(words, b)
        both = octets(mine, (16 * half, 16 * half + 8))
        edges = jnp.concatenate([plane(both, 4 * quarter + b) for b in range(4)], 0)
        reach = lax.dot_general(
            edges, near[...], (((1,), (1,)), ((), ())), preferred_element_type=F32
        )
        for b in range(4):
            scale = 1.0 / SCALE[4 * quarter + b]
            for k in range(2):
                at = 16 * half + 8 * k + 4 * quarter + b
                rows = slice(96 * b + 48 * k, 96 * b + 48 * k + 48)
                words = turned[pl.ds(at, 48, stride=32), :]
                low = (jnp.right_shift(words, lane) & 1).astype(F32)
                high = (jnp.right_shift(words, lane + 16) & 1).astype(F32)
                edge = (jnp.right_shift(mine, at) & 1).astype(F32)
                closed = jnp.sum(paths[rows, :] * edge, axis=1, keepdims=True)
                with_hub = jnp.sum(
                    reach[rows, :128] * low + reach[rows, 128:] * high, axis=1, keepdims=True
                )
                res[:, at : at + 1] = (0.5 * scale) * closed + scale * with_hub
                res[:, 32 + at : 33 + at] = first * jnp.sum(
                    edge[:, :768], axis=1, keepdims=True
                ) + once * jnp.sum(low + high, axis=1, keepdims=True)
    paths = jnp.dot(lhs[0, :256, :], rhs[...], preferred_element_type=F32)
    tri = jnp.concatenate(
        [
            jnp.sum(
                paths[32 * b + 8 * s : 32 * b + 8 * s + 8, :]
                * hub_col[64 * s + 8 * b : 64 * s + 8 * b + 8, :],
                axis=1,
                keepdims=True,
            )
            for s in range(4)
            for b in range(8)
        ],
        0,
    )
    bit = (lax.broadcasted_iota(I32, (256, 1), 0) // 8) & 7
    unscale = jnp.right_shift(128, bit).astype(F32) * jnp.where(bit == 7, -0.5 / 128, 0.5 / 128)
    hub_tri = unscale * tri
    hub_deg = first * jnp.sum(hub_col[:, :768], axis=1, keepdims=True)
    hub_part = lax.dot_general(
        wordhot,
        jnp.concatenate([hub_tri * bithot, hub_deg * bithot], 1),
        OUTER,
        precision=lax.Precision.HIGHEST,
        preferred_element_type=F32,
    )
    total = res[...] * jnp.concatenate([light, light], 1) + hub_part
    for c in range(16):
        line = jnp.concatenate(
            [total[3 * c + k : 3 * c + k + 1, 0:32] for k in range(3)]
            + [jnp.zeros((1, 32), F32)]
            + [total[3 * c + k : 3 * c + k + 1, 32:64] for k in range(3)]
            + [jnp.zeros((1, 32), F32)],
            1,
        )
        out[2 * c : 2 * c + 1, :] = line
        out[2 * c + 1 : 2 * c + 2, :] = line


def call(kernel, outs, scratch, args, flops, limit):
    vmem = pl.BlockSpec(memory_space=pltpu.VMEM)
    return pl.pallas_call(
        kernel,
        out_shape=[jax.ShapeDtypeStruct(*o) for o in outs],
        in_specs=[vmem] * len(args),
        out_specs=[vmem] * len(outs),
        scratch_shapes=scratch,
        cost_estimate=pl.CostEstimate(flops=flops, bytes_accessed=1 << 20, transcendentals=0),
        compiler_params=pltpu.CompilerParams(vmem_limit_bytes=limit * 2**20),
    )(*args)


def clustering(light_bits, hub_bits, hub_ids):
    _, _, _, _, zl = place()

    def send(value, source):
        return lax.ppermute(value, AXES, perm=permutation(source))

    rows = send(light_bits, fetch)
    beside = send(light_bits, partner)
    twin = send(hub_bits, lambda y, core, zh, x, zl: (y, core, zh, x, zl ^ 1))
    even = zl == 0
    hub = jnp.concatenate([jnp.where(even, hub_bits, twin), jnp.where(even, twin, hub_bits)], 0)
    hub_rows = send(hub, fetch)
    hub_beside = send(hub, partner)
    rows = jnp.concatenate([rows, hub_rows], 0)
    ring = [
        send(rows, lambda y, core, zh, x, zl, r=r: (y, core, zh, (x + r) % 4, zl))
        for r in (1, 3, 2)
    ]
    pair = jnp.concatenate([light_bits, beside], 0)
    hubs = jnp.concatenate([hub, hub_beside], 0)
    yy = send(pair, along_y)
    yc = send(yy, lambda y, core, zh, x, zl: (y, core ^ 1, zh, x, zl))
    planed = hub_ids.reshape(8, 32).T.reshape(256, 1)
    (rhs,) = call(right_kernel, [((3072, 1536), F8)], [], (yy, yc), 1 << 30, 8)
    (table,) = call(
        count_kernel,
        [((32, 256), F32)],
        [
            pltpu.VMEM((16, 768), I32),
            pltpu.VMEM((2, 384, 3072), F8),
            pltpu.VMEM((256, 1536), F8),
            pltpu.VMEM((1536, 128), I32),
            pltpu.VMEM((48, 64), F32),
        ],
        (planed, pair, hubs, rows, *ring, rhs),
        1 << 33,
        24,
    )
    everyone = lax.all_to_all(table, ("zh", "x", "zl"), 0, 0, tiled=True)
    total = jnp.sum(everyone, axis=0)
    return total[:OUT] / (1.0 + total[128 : 128 + OUT])


def solution(mesh):
    finer = Mesh(mesh.devices.reshape(SIZES), AXES)
    placed = (P(ROWS, COLS), P("zl", COLS), P())
    return jax.shard_map(
        clustering, mesh=finer, in_specs=placed, out_specs=P(ROWS + COLS), check_vma=False
    )
```

```python
import jax
import jax.numpy as jnp
from jax import lax
from jax.experimental import pallas as pl
from jax.experimental.pallas import tpu as pltpu
from jax.sharding import Mesh
from jax.sharding import PartitionSpec as P

AXES = ("y", "core", "zh", "x", "zl")
ROWS = ("y", "core")
COLS = ("zh", "x")
SIZES = (4, 2, 4, 4, 2)
F8 = jnp.float8_e4m3fn
F32 = jnp.float32
I32 = jnp.int32
I8 = jnp.int8
BF16 = jnp.bfloat16
OUT = 96


def flat(y, core, zh, x, zl):
    return (((y * 2 + core) * 4 + zh) * 4 + x) * 2 + zl


def permutation(source_of):
    pairs = []
    for y in range(4):
        for core in range(2):
            for zh in range(4):
                for x in range(4):
                    for zl in range(2):
                        s = source_of(y, core, zh, x, zl)
                        if s is not None:
                            pairs.append((flat(*s), flat(y, core, zh, x, zl)))
    return pairs


FETCH = ((0, 1, 0, 1), (1, 0, 0, 1), (1, 0, 1, 0), (1, 0, 0, 1))


def group_of(y, z):
    return (-(y + z)) & 3


def fetch(y, core, zh, x, zl):
    z = 2 * zh + zl
    group = group_of(y, z)
    return (y, core, group, x, FETCH[(-y) & 3][group] ^ (z >> 2))


def partner(y, core, zh, x, zl):
    return (y, core, (zh + 1) % 4, x, 0) if zl == 1 else (y, core, (zh + 3) % 4, x, 1)


def along_y(y, core, zh, x, zl):
    return (group_of(y, 2 * zh + zl), core, zh, x, zl)


def unpack(words):
    n = words.shape[1]
    shifts = lax.broadcasted_iota(I32, (32, n), 0)
    rows = [
        jnp.right_shift(jnp.broadcast_to(words[i : i + 1, :], (32, n)), shifts)
        for i in range(words.shape[0])
    ]
    bits = jnp.concatenate(rows, 0).astype(I8) & I8(1)
    return bits.astype(BF16).astype(F8)


def place():
    y, core = lax.axis_index("y"), lax.axis_index("core")
    zh, x, zl = lax.axis_index("zh"), lax.axis_index("x"), lax.axis_index("zl")
    return y, core, zh, x, zl


def octets(words, at):
    return jnp.concatenate([jnp.right_shift(words, a) for a in at], 0).astype(I8)


def plane(bytes8, b):
    return (bytes8 & I8(SCALE[b])).astype(BF16).astype(F8)


SCALE = (1, 2, 4, 8, 16, 32, 64, -128)
OUTER = (((0,), (0,)), ((), ()))


def right_kernel(yy, yc, rhs):
    _, core, _, x, _ = place()
    for n, rel in enumerate((0, 1, 3, 2)):
        xs = lax.rem(x + rel, 4)
        other = (xs // 2) != core
        for side in range(2):
            at = pl.multiple_of(48 * side + 24 * lax.rem(xs, 2), 8)
            words = jnp.where(other, yc[pl.ds(at, 24), :], yy[pl.ds(at, 24), :])
            for part in range(3):
                base = 768 * n + 256 * part
                rhs[base : base + 256, 768 * side : 768 * side + 768] = unpack(
                    words[8 * part : 8 * part + 8, :]
                )


def prep_kernel(idp, pair, hubs, keep, mine, near, light, deg):
    y, core, zh, x, zl = place()
    row = 2 * y + core
    ids = idp[...]
    q = (lax.broadcasted_iota(I32, (256, 16), 1) == ids // 768).astype(BF16)
    r = (lax.broadcasted_iota(I32, (256, 768), 1) == ids % 768).astype(BF16)
    keep[...] = jnp.where(lax.dot_general(q, r, OUTER, preferred_element_type=F32) > 0.5, 0, -1)
    wordhot = (lax.broadcasted_iota(I32, (256, 48), 1) + 48 * row == ids // 32).astype(BF16)
    bithot = (lax.broadcasted_iota(I32, (256, 32), 1) == ids % 32).astype(BF16)
    light[...] = 1.0 - lax.dot_general(wordhot, bithot, OUTER, preferred_element_type=F32)
    own = pl.ds(4 * zh + x, 1)
    side = pl.ds(4 * ((zh + 3 + 2 * zl) & 3) + x, 1)
    left = pair[0:48, :] & keep[own, :]
    mine[:, 0:768] = left
    mine[:, 768:1536] = pair[48:96, :] & keep[side, :]
    for part, line in enumerate((own, side)):
        words = hubs[8 * part : 8 * part + 8, :] & keep[line, :]
        for b in range(8):
            bits = octets(words, (b, 8 + b, 16 + b, 24 + b)) & I8(1)
            near[32 * b : 32 * b + 32, 768 * part : 768 * part + 768] = bits.astype(
                BF16
            ).astype(F8)
    first = (zl == 0).astype(F32)
    for at in range(32):
        edge = (jnp.right_shift(left, at) & 1).astype(F32)
        deg[:, at : at + 1] = jnp.sum(edge, axis=1, keepdims=True)
    hub_deg = jnp.sum(near[:, 0:768].astype(F32), axis=1, keepdims=True)
    hub_deg = lax.dot_general(
        wordhot.astype(F32),
        hub_deg * bithot.astype(F32),
        OUTER,
        precision=lax.Precision.HIGHEST,
        preferred_element_type=F32,
    )
    deg[...] = first * (deg[...] * light[...] + hub_deg)


def count_kernel(idp, keep, mine, near, light, deg, r0, rp, rm, r2, rhs, out, lhs, turned, res):
    y, core, zh, x, zl = place()
    row = 2 * y + core
    z = 2 * zh + zl
    group = (16 - y - z) & 3
    sources = ((r0, 0), (rp, 1), (rm, 3), (r2, 2))
    for side in range(2):
        xs = 2 * core + side
        words = jnp.zeros((8, 768), I32)
        for ref, rel in sources:
            hit = (lax.rem(x + rel, 4) == xs) & (group == y)
            words = jnp.where(hit, ref[48:56, :], words)
        words = words & keep[pl.ds(2 * row + side, 1), :]
        turned[768 * side : 768 * side + 768, :] = jnp.concatenate([words] * 16, 0).T
    lane = lax.broadcasted_iota(I32, (48, 128), 1)
    lane = 8 * ((lane // 8) & 3) + lane // 32
    once = ((x == 0) & (z == ((16 - 2 * y) & 3))).astype(F32)

    def masked(ref, rel, rows):
        return ref[rows, :] & keep[pl.ds(4 * group + lax.rem(x + rel, 4), 1), :]

    def fill(tile):
        half, quarter = tile // 2, tile % 2
        for n, (ref, rel) in enumerate(sources):
            words = masked(ref, rel, slice(0, 48))
            both = octets(words, (16 * half, 16 * half + 8))
            for b in range(4):
                lhs[tile % 2, 96 * b : 96 * b + 96, 768 * n : 768 * n + 768] = plane(
                    both, 4 * quarter + b
                )

    fill(0)
    for tile in range(4):
        half, quarter = tile // 2, tile % 2
        paths = jnp.dot(lhs[tile % 2], rhs[...], preferred_element_type=F32)
        if tile < 3:
            fill(tile + 1)
        else:
            for n, (ref, rel) in enumerate(sources):
                words = octets(masked(ref, rel, slice(48, 56)), (0, 8, 16, 24))
                for b in range(8):
                    lhs[0, 32 * b : 32 * b + 32, 768 * n : 768 * n + 768] = plane(words, b)
        both = octets(mine[...], (16 * half, 16 * half + 8))
        edges = jnp.concatenate([plane(both, 4 * quarter + b) for b in range(4)], 0)
        reach = lax.dot_general(
            edges, near[...], (((1,), (1,)), ((), ())), preferred_element_type=F32
        )
        for b in range(4):
            scale = 1.0 / SCALE[4 * quarter + b]
            for k in range(2):
                at = 16 * half + 8 * k + 4 * quarter + b
                rows = slice(96 * b + 48 * k, 96 * b + 48 * k + 48)
                words = turned[pl.ds(at, 48, stride=32), :]
                low = (jnp.right_shift(words, lane) & 1).astype(F32)
                high = (jnp.right_shift(words, lane + 4) & 1).astype(F32)
                edge = (jnp.right_shift(mine[...], at) & 1).astype(F32)
                closed = jnp.sum(paths[rows, :] * edge, axis=1, keepdims=True)
                with_hub = jnp.sum(
                    reach[rows, :128] * low + reach[rows, 128:] * high, axis=1, keepdims=True
                )
                res[:, at : at + 1] = (0.5 * scale) * closed + scale * with_hub
                res[:, 32 + at : 33 + at] = once * jnp.sum(low + high, axis=1, keepdims=True)
    paths = jnp.dot(lhs[0, :256, :], rhs[...], preferred_element_type=F32)
    bit = lax.broadcasted_iota(I32, (256, 1), 0) // 32
    unscale = jnp.right_shift(128, bit).astype(F32) * jnp.where(bit == 7, -0.5 / 128, 0.5 / 128)
    hub_tri = unscale * jnp.sum(paths * near[...].astype(F32), axis=1, keepdims=True)
    ids = idp[...]
    wordhot = (lax.broadcasted_iota(I32, (256, 48), 1) + 48 * row == ids // 32).astype(F32)
    bithot = (lax.broadcasted_iota(I32, (256, 32), 1) == ids % 32).astype(F32)
    hub_tri = lax.dot_general(
        wordhot,
        hub_tri * bithot,
        OUTER,
        precision=lax.Precision.HIGHEST,
        preferred_element_type=F32,
    )
    total = jnp.concatenate(
        [res[:, 0:32] * light[...] + hub_tri, res[:, 32:64] * light[...] + deg[...]], 1
    )
    for c in range(16):
        line = jnp.concatenate(
            [total[3 * c + k : 3 * c + k + 1, 0:32] for k in range(3)]
            + [jnp.zeros((1, 32), F32)]
            + [total[3 * c + k : 3 * c + k + 1, 32:64] for k in range(3)]
            + [jnp.zeros((1, 32), F32)],
            1,
        )
        out[c : c + 1, :] = line


def call(kernel, outs, scratch, args, flops, limit):
    vmem = pl.BlockSpec(memory_space=pltpu.VMEM)
    return pl.pallas_call(
        kernel,
        out_shape=[jax.ShapeDtypeStruct(*o) for o in outs],
        in_specs=[vmem] * len(args),
        out_specs=[vmem] * len(outs),
        scratch_shapes=scratch,
        cost_estimate=pl.CostEstimate(flops=flops, bytes_accessed=1 << 20, transcendentals=0),
        compiler_params=pltpu.CompilerParams(vmem_limit_bytes=limit * 2**20),
    )(*args)


def clustering(light_bits, hub_bits, hub_ids):
    _, _, _, _, zl = place()

    def send(value, source):
        return lax.ppermute(value, AXES, perm=permutation(source))

    rows = send(light_bits, fetch)
    beside = send(light_bits, partner)
    twin = send(hub_bits, lambda y, core, zh, x, zl: (y, core, zh, x, zl ^ 1))
    even = zl == 0
    hub = jnp.concatenate([jnp.where(even, hub_bits, twin), jnp.where(even, twin, hub_bits)], 0)
    hub_rows = send(hub, fetch)
    hub_beside = send(hub, partner)
    rows = jnp.concatenate([rows, hub_rows], 0)
    ring = [
        send(rows, lambda y, core, zh, x, zl, r=r: (y, core, zh, (x + r) % 4, zl))
        for r in (1, 3, 2)
    ]
    pair = jnp.concatenate([light_bits, beside], 0)
    hubs = jnp.concatenate([hub, hub_beside], 0)
    yy = send(pair, along_y)
    yc = send(yy, lambda y, core, zh, x, zl: (y, core ^ 1, zh, x, zl))
    planed = hub_ids.reshape(8, 4, 8).transpose(2, 1, 0).reshape(256, 1)
    ready = call(
        prep_kernel,
        [((16, 768), I32), ((48, 1536), I32), ((256, 1536), F8), ((48, 32), F32), ((48, 32), F32)],
        [],
        (planed, pair, hubs),
        1 << 30,
        8,
    )
    (rhs,) = call(right_kernel, [((3072, 1536), F8)], [], (yy, yc), 1 << 30, 8)
    (table,) = call(
        count_kernel,
        [((16, 256), F32)],
        [pltpu.VMEM((2, 384, 3072), F8), pltpu.VMEM((1536, 128), I32), pltpu.VMEM((48, 64), F32)],
        (planed, *ready, rows, *ring, rhs),
        1 << 33,
        24,
    )
    everyone = lax.all_to_all(table, ("zh", "x"), 0, 0, tiled=True)
    total = jnp.sum(everyone, axis=0, keepdims=True)
    total = (total + lax.ppermute(total, "zl", [(0, 1), (1, 0)]))[0]
    return total[:OUT] / (1.0 + total[128 : 128 + OUT])


def solution(mesh):
    finer = Mesh(mesh.devices.reshape(SIZES), AXES)
    placed = (P(ROWS, COLS), P("zl", COLS), P())
    return jax.shard_map(
        clustering, mesh=finer, in_specs=placed, out_specs=P(ROWS + COLS), check_vma=False
    )
```

```python
import jax
import jax.numpy as jnp
from jax import lax
from jax.experimental import pallas as pl
from jax.experimental.pallas import tpu as pltpu
from jax.sharding import Mesh
from jax.sharding import PartitionSpec as P

AXES = ("y", "core", "zh", "x", "zl")
ROWS = ("y", "core")
COLS = ("zh", "x")
SIZES = (4, 2, 4, 4, 2)
F8 = jnp.float8_e4m3fn
F32 = jnp.float32
I32 = jnp.int32
I8 = jnp.int8
BF16 = jnp.bfloat16
OUT = 96


def flat(y, core, zh, x, zl):
    return (((y * 2 + core) * 4 + zh) * 4 + x) * 2 + zl


def permutation(source_of):
    pairs = []
    for y in range(4):
        for core in range(2):
            for zh in range(4):
                for x in range(4):
                    for zl in range(2):
                        s = source_of(y, core, zh, x, zl)
                        if s is not None:
                            pairs.append((flat(*s), flat(y, core, zh, x, zl)))
    return pairs


FETCH = ((0, 1, 0, 1), (1, 0, 0, 1), (1, 0, 1, 0), (1, 0, 0, 1))
FETCH_BITS = sum(bit << (4 * r + g) for r, line in enumerate(FETCH) for g, bit in enumerate(line))


def group_of(y, z):
    return (-(y + z)) & 3


def fetch(y, core, zh, x, zl):
    z = 2 * zh + zl
    group = group_of(y, z)
    return (y, core, group, x, FETCH[(-y) & 3][group] ^ (z >> 2))


def partner(y, core, zh, x, zl):
    return (y, core, (zh + 1) % 4, x, 0) if zl == 1 else (y, core, (zh + 3) % 4, x, 1)


def along_y(y, core, zh, x, zl):
    return (group_of(y, 2 * zh + zl), core, zh, x, zl)


def unpack(words):
    n = words.shape[1]
    shifts = lax.broadcasted_iota(I32, (32, n), 0)
    rows = [
        jnp.right_shift(jnp.broadcast_to(words[i : i + 1, :], (32, n)), shifts)
        for i in range(words.shape[0])
    ]
    bits = jnp.concatenate(rows, 0).astype(I8) & I8(1)
    return bits.astype(BF16).astype(F8)


def place():
    y, core = lax.axis_index("y"), lax.axis_index("core")
    zh, x, zl = lax.axis_index("zh"), lax.axis_index("x"), lax.axis_index("zl")
    return y, core, zh, x, zl


def planes(words, bits):
    return jnp.concatenate([jnp.right_shift(words, b) & 1 for b in bits], 0)


def octets(words, at):
    return jnp.concatenate([jnp.right_shift(words, a) for a in at], 0).astype(I8)


def plane(bytes8, b):
    return (bytes8 & I8(SCALE[b])).astype(BF16).astype(F8)


SCALE = (1, 2, 4, 8, 16, 32, 64, -128)
OUTER = (((0,), (0,)), ((), ()))


def by_group(words, first):
    return jnp.where(first == 1, jnp.concatenate([words[4:8], words[0:4]], 0), words)


def right_kernel(words, rhs):
    for side in range(2):
        for part in range(6):
            rhs[256 * part : 256 * part + 256, 768 * side : 768 * side + 768] = unpack(
                words[48 * side + 8 * part : 48 * side + 8 * part + 8, :]
            )


def count_kernel(
    idp, pair, hubs, r0, rp, rm, r2, mine_rhs, other_rhs, out, keep, bits, lhs, near, turned, res
):
    y, core, zh, x, zl = place()
    row = 2 * y + core
    z = 2 * zh + zl
    group = (16 - y - z) & 3
    sources = ((r0, 0), (rp, 1), (rm, 3), (r2, 2))
    ids = idp[...]
    q = (lax.broadcasted_iota(I32, (256, 16), 1) == ids // 768).astype(BF16)
    r = (lax.broadcasted_iota(I32, (256, 768), 1) == ids % 768).astype(BF16)
    keep[...] = jnp.where(lax.dot_general(q, r, OUTER, preferred_element_type=F32) > 0.5, 0, -1)
    wordhot = (lax.broadcasted_iota(I32, (256, 48), 1) + 48 * row == ids // 32).astype(F32)
    bithot = (lax.broadcasted_iota(I32, (256, 32), 1) == ids % 32).astype(F32)
    light = 1.0 - lax.dot_general(
        wordhot.astype(BF16), bithot.astype(BF16), OUTER, preferred_element_type=F32
    )
    own = pl.ds(4 * zh + x, 1)
    side = pl.ds(4 * ((zh + 3 + 2 * zl) & 3) + x, 1)
    mine = jnp.concatenate([pair[0:48, :] & keep[own, :], pair[48:96, :] & keep[side, :]], 1)
    hub_words = jnp.concatenate(
        [
            by_group(hubs[0:8, :], zl) & keep[own, :],
            by_group(hubs[8:16, :], 1 - zl) & keep[side, :],
        ],
        1,
    )
    turn = jnp.right_shift(FETCH_BITS, 4 * ((4 - y) & 3) + group) & 1
    sent_by = turn ^ (z // 4)
    hub_col = planes(hub_words, range(32)).astype(F32)
    near[...] = hub_col.astype(F8)
    for p in range(4):
        xs = 2 * (core ^ (p // 2)) + p % 2
        rel = (4 + xs - x) & 3
        words = r0[...]
        for ref, k in sources[1:]:
            words = jnp.where(rel == k, ref[...], words)
        hub_rows = by_group(words[48:], sent_by)
        if p < 2:
            found = jnp.where(group == y, hub_rows, 0) & keep[pl.ds(2 * row + p, 1), :]
            turned[768 * p : 768 * p + 768, :] = jnp.concatenate([found] * 16, 0).T
        line = keep[pl.ds(4 * group + xs, 1), :]
        bits[56 * p : 56 * p + 48, :] = words[:48] & line
        bits[56 * p + 48 : 56 * p + 56, :] = hub_rows & line
    lane = lax.broadcasted_iota(I32, (48, 128), 1) // 8
    first = (zl == 0).astype(F32)
    once = ((x == 0) & (z == ((16 - 2 * y) & 3))).astype(F32)

    def fill(tile):
        for p in range(4):
            at = slice(768 * p, 768 * p + 768)
            if tile < 0:
                words = octets(bits[56 * p + 48 : 56 * p + 56, :], (0, 8, 16, 24))
                for b in range(8):
                    lhs[1, 32 * b : 32 * b + 32, at] = plane(words, b)
            else:
                half, quarter = tile // 2, tile % 2
                words = octets(bits[56 * p : 56 * p + 48, :], (16 * half, 16 * half + 8))
                for b in range(4):
                    lhs[tile % 2, 96 * b : 96 * b + 96, at] = plane(words, 4 * quarter + b)

    def product(tile, size):
        return jnp.dot(
            lhs[tile % 2, :size, :1536], mine_rhs[...], preferred_element_type=F32
        ) + jnp.dot(lhs[tile % 2, :size, 1536:], other_rhs[...], preferred_element_type=F32)

    fill(-1)
    hub_paths = product(-1, 256)
    fill(0)
    hub_tri = jnp.concatenate(
        [
            jnp.sum(
                hub_paths[32 * b + 8 * s : 32 * b + 8 * s + 8, :]
                * hub_col[64 * s + 8 * b : 64 * s + 8 * b + 8, :],
                axis=1,
                keepdims=True,
            )
            for s in range(4)
            for b in range(8)
        ],
        0,
    )
    bit = (lax.broadcasted_iota(I32, (256, 1), 0) // 8) & 7
    unscale = jnp.right_shift(128, bit).astype(F32) * jnp.where(bit == 7, -0.5 / 128, 0.5 / 128)
    hub_tri = unscale * hub_tri
    hub_deg = first * jnp.sum(hub_col[:, :768], axis=1, keepdims=True)
    hub_part = lax.dot_general(
        wordhot,
        jnp.concatenate([hub_tri * bithot, hub_deg * bithot], 1),
        OUTER,
        precision=lax.Precision.HIGHEST,
        preferred_element_type=F32,
    )
    for tile in range(4):
        half, quarter = tile // 2, tile % 2
        paths = product(tile, 384)
        if tile < 3:
            fill(tile + 1)
        both = octets(mine, (16 * half, 16 * half + 8))
        edges = jnp.concatenate([plane(both, 4 * quarter + b) for b in range(4)], 0)
        reach = lax.dot_general(
            edges, near[...], (((1,), (1,)), ((), ())), preferred_element_type=F32
        )
        for b in range(4):
            scale = 1.0 / SCALE[4 * quarter + b]
            for k in range(2):
                at = 16 * half + 8 * k + 4 * quarter + b
                rows = slice(96 * b + 48 * k, 96 * b + 48 * k + 48)
                words = turned[pl.ds(at, 48, stride=32), :]
                low = (jnp.right_shift(words, lane) & 1).astype(F32)
                high = (jnp.right_shift(words, lane + 16) & 1).astype(F32)
                edge = (jnp.right_shift(mine, at) & 1).astype(F32)
                closed = jnp.sum(paths[rows, :] * edge, axis=1, keepdims=True)
                with_hub = jnp.sum(
                    reach[rows, :128] * low + reach[rows, 128:] * high, axis=1, keepdims=True
                )
                res[:, at : at + 1] = (0.5 * scale) * closed + scale * with_hub
                res[:, 32 + at : 33 + at] = first * jnp.sum(
                    edge[:, :768], axis=1, keepdims=True
                ) + once * jnp.sum(low + high, axis=1, keepdims=True)
    total = res[...] * jnp.concatenate([light, light], 1) + hub_part
    for c in range(16):
        line = jnp.concatenate(
            [total[3 * c + k : 3 * c + k + 1, 0:32] for k in range(3)]
            + [jnp.zeros((1, 32), F32)]
            + [total[3 * c + k : 3 * c + k + 1, 32:64] for k in range(3)]
            + [jnp.zeros((1, 32), F32)],
            1,
        )
        out[2 * c : 2 * c + 1, :] = line
        out[2 * c + 1 : 2 * c + 2, :] = line


def call(kernel, outs, scratch, args, flops, limit):
    vmem = pl.BlockSpec(memory_space=pltpu.VMEM)
    return pl.pallas_call(
        kernel,
        out_shape=[jax.ShapeDtypeStruct(*o) for o in outs],
        in_specs=[vmem] * len(args),
        out_specs=[vmem] * len(outs),
        scratch_shapes=scratch,
        cost_estimate=pl.CostEstimate(flops=flops, bytes_accessed=1 << 20, transcendentals=0),
        compiler_params=pltpu.CompilerParams(vmem_limit_bytes=limit * 2**20),
    )(*args)


def clustering(light_bits, hub_bits, hub_ids):
    def send(value, source):
        return lax.ppermute(value, AXES, perm=permutation(source))

    rows = send(light_bits, fetch)
    beside = send(light_bits, partner)
    twin = send(hub_bits, lambda y, core, zh, x, zl: (y, core, zh, x, zl ^ 1))
    hub = jnp.concatenate([hub_bits, twin], 0)
    hub_rows = send(hub, fetch)
    hub_beside = send(hub, partner)
    rows = jnp.concatenate([rows, hub_rows], 0)
    ring = [
        send(rows, lambda y, core, zh, x, zl, r=r: (y, core, zh, (x + r) % 4, zl))
        for r in (1, 3, 2)
    ]
    pair = jnp.concatenate([light_bits, beside], 0)
    hubs = jnp.concatenate([hub, hub_beside], 0)
    yy = send(pair, along_y)
    yc = send(yy, lambda y, core, zh, x, zl: (y, core ^ 1, zh, x, zl))
    planed = hub_ids.reshape(8, 32).T.reshape(256, 1)
    sides = []
    for words in (yy, yc):
        sides += call(right_kernel, [((1536, 1536), F8)], [], (words,), 1 << 29, 8)
    (table,) = call(
        count_kernel,
        [((32, 256), F32)],
        [
            pltpu.VMEM((16, 768), I32),
            pltpu.VMEM((224, 768), I32),
            pltpu.VMEM((2, 384, 3072), F8),
            pltpu.VMEM((256, 1536), F8),
            pltpu.VMEM((1536, 128), I32),
            pltpu.VMEM((48, 64), F32),
        ],
        (planed, pair, hubs, rows, *ring, *sides),
        1 << 33,
        24,
    )
    everyone = lax.all_to_all(table, ("zh", "x", "zl"), 0, 0, tiled=True)
    total = jnp.sum(everyone, axis=0)
    return total[:OUT] / (1.0 + total[128 : 128 + OUT])


def solution(mesh):
    finer = Mesh(mesh.devices.reshape(SIZES), AXES)
    placed = (P(ROWS, COLS), P("zl", COLS), P())
    return jax.shard_map(
        clustering, mesh=finer, in_specs=placed, out_specs=P(ROWS + COLS), check_vma=False
    )
```

```python
import jax
import jax.numpy as jnp
from jax import lax
from jax.experimental import pallas as pl
from jax.experimental.pallas import tpu as pltpu
from jax.sharding import Mesh
from jax.sharding import PartitionSpec as P

AXES = ("y", "core", "zh", "x", "zl")
ROWS = ("y", "core")
COLS = ("zh", "x")
SIZES = (4, 2, 4, 4, 2)
F8 = jnp.float8_e4m3fn
F32 = jnp.float32
I32 = jnp.int32
I8 = jnp.int8
BF16 = jnp.bfloat16
OUT = 96


def flat(y, core, zh, x, zl):
    return (((y * 2 + core) * 4 + zh) * 4 + x) * 2 + zl


def permutation(source_of):
    pairs = []
    for y in range(4):
        for core in range(2):
            for zh in range(4):
                for x in range(4):
                    for zl in range(2):
                        s = source_of(y, core, zh, x, zl)
                        if s is not None:
                            pairs.append((flat(*s), flat(y, core, zh, x, zl)))
    return pairs


FETCH = ((0, 1, 0, 1), (1, 0, 0, 1), (1, 0, 1, 0), (1, 0, 0, 1))


def group_of(y, z):
    return (-(y + z)) & 3


def fetch(y, core, zh, x, zl):
    z = 2 * zh + zl
    group = group_of(y, z)
    return (y, core, group, x, FETCH[(-y) & 3][group] ^ (z >> 2))


def partner(y, core, zh, x, zl):
    return (y, core, (zh + 1) % 4, x, 0) if zl == 1 else (y, core, (zh + 3) % 4, x, 1)


def along_y(y, core, zh, x, zl):
    return (group_of(y, 2 * zh + zl), core, zh, x, zl)


def unpack(words):
    n = words.shape[1]
    shifts = lax.broadcasted_iota(I32, (32, n), 0)
    rows = [
        jnp.right_shift(jnp.broadcast_to(words[i : i + 1, :], (32, n)), shifts)
        for i in range(words.shape[0])
    ]
    bits = jnp.concatenate(rows, 0).astype(I8) & I8(1)
    return bits.astype(BF16).astype(F8)


def place():
    y, core = lax.axis_index("y"), lax.axis_index("core")
    zh, x, zl = lax.axis_index("zh"), lax.axis_index("x"), lax.axis_index("zl")
    return y, core, zh, x, zl


def planes(words, bits):
    return jnp.concatenate([jnp.right_shift(words, b) & 1 for b in bits], 0)


def octets(words, at):
    return jnp.concatenate([jnp.right_shift(words, a) for a in at], 0).astype(I8)


def plane(bytes8, b):
    return (bytes8 & I8(SCALE[b])).astype(BF16).astype(F8)


SCALE = (1, 2, 4, 8, 16, 32, 64, -128)
OUTER = (((0,), (0,)), ((), ()))


def right_kernel(words, rhs):
    for side in range(2):
        for part in range(6):
            rhs[256 * part : 256 * part + 256, 768 * side : 768 * side + 768] = unpack(
                words[48 * side + 8 * part : 48 * side + 8 * part + 8, :]
            )


def count_kernel(
    idp, pair, hubs, r0, rp, rm, r2, mine_rhs, other_rhs, out, keep, bits, lhs, near, turned, res
):
    y, core, zh, x, zl = place()
    row = 2 * y + core
    z = 2 * zh + zl
    group = (16 - y - z) & 3
    sources = ((r0, 0), (rp, 1), (rm, 3), (r2, 2))
    ids = idp[...]
    q = (lax.broadcasted_iota(I32, (256, 16), 1) == ids // 768).astype(BF16)
    r = (lax.broadcasted_iota(I32, (256, 768), 1) == ids % 768).astype(BF16)
    keep[...] = jnp.where(lax.dot_general(q, r, OUTER, preferred_element_type=F32) > 0.5, 0, -1)
    wordhot = (lax.broadcasted_iota(I32, (256, 48), 1) + 48 * row == ids // 32).astype(F32)
    bithot = (lax.broadcasted_iota(I32, (256, 32), 1) == ids % 32).astype(F32)
    light = 1.0 - lax.dot_general(
        wordhot.astype(BF16), bithot.astype(BF16), OUTER, preferred_element_type=F32
    )
    own = pl.ds(4 * zh + x, 1)
    side = pl.ds(4 * ((zh + 3 + 2 * zl) & 3) + x, 1)
    mine = jnp.concatenate([pair[0:48, :] & keep[own, :], pair[48:96, :] & keep[side, :]], 1)
    hub_words = jnp.concatenate(
        [hubs[0:8, :] & keep[own, :], hubs[8:16, :] & keep[side, :]], 1
    )
    hub_col = planes(hub_words, range(32)).astype(F32)
    near[...] = hub_col.astype(F8)
    for p in range(4):
        xs = 2 * (core ^ (p // 2)) + p % 2
        rel = (4 + xs - x) & 3
        words = r0[...]
        for ref, k in sources[1:]:
            words = jnp.where(rel == k, ref[...], words)
        if p < 2:
            found = jnp.where(group == y, words[48:], 0) & keep[pl.ds(2 * row + p, 1), :]
            turned[768 * p : 768 * p + 768, :] = jnp.concatenate([found] * 16, 0).T
        bits[56 * p : 56 * p + 56, :] = words & keep[pl.ds(4 * group + xs, 1), :]
    lane = lax.broadcasted_iota(I32, (48, 128), 1) // 8
    first = (zl == 0).astype(F32)
    once = ((x == 0) & (z == ((16 - 2 * y) & 3))).astype(F32)

    def fill(tile):
        for p in range(4):
            at = slice(768 * p, 768 * p + 768)
            if tile < 0:
                words = octets(bits[56 * p + 48 : 56 * p + 56, :], (0, 8, 16, 24))
                for b in range(8):
                    lhs[1, 32 * b : 32 * b + 32, at] = plane(words, b)
            else:
                half, quarter = tile // 2, tile % 2
                words = octets(bits[56 * p : 56 * p + 48, :], (16 * half, 16 * half + 8))
                for b in range(4):
                    lhs[tile % 2, 96 * b : 96 * b + 96, at] = plane(words, 4 * quarter + b)

    def product(tile, size):
        return jnp.dot(
            lhs[tile % 2, :size, :1536], mine_rhs[...], preferred_element_type=F32
        ) + jnp.dot(lhs[tile % 2, :size, 1536:], other_rhs[...], preferred_element_type=F32)

    fill(-1)
    hub_paths = product(-1, 256)
    fill(0)
    hub_tri = jnp.concatenate(
        [
            jnp.sum(
                hub_paths[32 * b + 8 * s : 32 * b + 8 * s + 8, :]
                * hub_col[64 * s + 8 * b : 64 * s + 8 * b + 8, :],
                axis=1,
                keepdims=True,
            )
            for s in range(4)
            for b in range(8)
        ],
        0,
    )
    bit = (lax.broadcasted_iota(I32, (256, 1), 0) // 8) & 7
    unscale = jnp.right_shift(128, bit).astype(F32) * jnp.where(bit == 7, -0.5 / 128, 0.5 / 128)
    hub_tri = unscale * hub_tri
    hub_deg = first * jnp.sum(hub_col[:, :768], axis=1, keepdims=True)
    hub_part = lax.dot_general(
        wordhot,
        jnp.concatenate([hub_tri * bithot, hub_deg * bithot], 1),
        OUTER,
        precision=lax.Precision.HIGHEST,
        preferred_element_type=F32,
    )
    for tile in range(4):
        half, quarter = tile // 2, tile % 2
        paths = product(tile, 384)
        if tile < 3:
            fill(tile + 1)
        both = octets(mine, (16 * half, 16 * half + 8))
        edges = jnp.concatenate([plane(both, 4 * quarter + b) for b in range(4)], 0)
        reach = lax.dot_general(
            edges, near[...], (((1,), (1,)), ((), ())), preferred_element_type=F32
        )
        for b in range(4):
            scale = 1.0 / SCALE[4 * quarter + b]
            for k in range(2):
                at = 16 * half + 8 * k + 4 * quarter + b
                rows = slice(96 * b + 48 * k, 96 * b + 48 * k + 48)
                words = turned[pl.ds(at, 48, stride=32), :]
                low = (jnp.right_shift(words, lane) & 1).astype(F32)
                high = (jnp.right_shift(words, lane + 16) & 1).astype(F32)
                edge = (jnp.right_shift(mine, at) & 1).astype(F32)
                closed = jnp.sum(paths[rows, :] * edge, axis=1, keepdims=True)
                with_hub = jnp.sum(
                    reach[rows, :128] * low + reach[rows, 128:] * high, axis=1, keepdims=True
                )
                res[:, at : at + 1] = (0.5 * scale) * closed + scale * with_hub
                res[:, 32 + at : 33 + at] = first * jnp.sum(
                    edge[:, :768], axis=1, keepdims=True
                ) + once * jnp.sum(low + high, axis=1, keepdims=True)
    total = res[...] * jnp.concatenate([light, light], 1) + hub_part
    for c in range(16):
        line = jnp.concatenate(
            [total[3 * c + k : 3 * c + k + 1, 0:32] for k in range(3)]
            + [jnp.zeros((1, 32), F32)]
            + [total[3 * c + k : 3 * c + k + 1, 32:64] for k in range(3)]
            + [jnp.zeros((1, 32), F32)],
            1,
        )
        out[2 * c : 2 * c + 1, :] = line
        out[2 * c + 1 : 2 * c + 2, :] = line


def call(kernel, outs, scratch, args, flops, limit):
    vmem = pl.BlockSpec(memory_space=pltpu.VMEM)
    return pl.pallas_call(
        kernel,
        out_shape=[jax.ShapeDtypeStruct(*o) for o in outs],
        in_specs=[vmem] * len(args),
        out_specs=[vmem] * len(outs),
        scratch_shapes=scratch,
        cost_estimate=pl.CostEstimate(flops=flops, bytes_accessed=1 << 20, transcendentals=0),
        compiler_params=pltpu.CompilerParams(vmem_limit_bytes=limit * 2**20),
    )(*args)


def clustering(light_bits, hub_bits, hub_ids):
    _, _, _, _, zl = place()

    def send(value, source):
        return lax.ppermute(value, AXES, perm=permutation(source))

    rows = send(light_bits, fetch)
    beside = send(light_bits, partner)
    twin = send(hub_bits, lambda y, core, zh, x, zl: (y, core, zh, x, zl ^ 1))
    even = zl == 0
    hub = jnp.concatenate([jnp.where(even, hub_bits, twin), jnp.where(even, twin, hub_bits)], 0)
    hub_rows = send(hub, fetch)
    hub_beside = send(hub, partner)
    rows = jnp.concatenate([rows, hub_rows], 0)
    ring = [
        send(rows, lambda y, core, zh, x, zl, r=r: (y, core, zh, (x + r) % 4, zl))
        for r in (1, 3, 2)
    ]
    pair = jnp.concatenate([light_bits, beside], 0)
    hubs = jnp.concatenate([hub, hub_beside], 0)
    yy = send(pair, along_y)
    yc = send(yy, lambda y, core, zh, x, zl: (y, core ^ 1, zh, x, zl))
    planed = hub_ids.reshape(8, 32).T.reshape(256, 1)
    sides = []
    for words in (yy, yc):
        sides += call(right_kernel, [((1536, 1536), F8)], [], (words,), 1 << 29, 8)
    (table,) = call(
        count_kernel,
        [((32, 256), F32)],
        [
            pltpu.VMEM((16, 768), I32),
            pltpu.VMEM((224, 768), I32),
            pltpu.VMEM((2, 384, 3072), F8),
            pltpu.VMEM((256, 1536), F8),
            pltpu.VMEM((1536, 128), I32),
            pltpu.VMEM((48, 64), F32),
        ],
        (planed, pair, hubs, rows, *ring, *sides),
        1 << 33,
        24,
    )
    everyone = lax.all_to_all(table, ("zh", "x", "zl"), 0, 0, tiled=True)
    total = jnp.sum(everyone, axis=0)
    return total[:OUT] / (1.0 + total[128 : 128 + OUT])


def solution(mesh):
    finer = Mesh(mesh.devices.reshape(SIZES), AXES)
    placed = (P(ROWS, COLS), P("zl", COLS), P())
    return jax.shard_map(
        clustering, mesh=finer, in_specs=placed, out_specs=P(ROWS + COLS), check_vma=False
    )
```
